1024 devices in a mesh: exp: 64 (over z, x), head: 16 (over y, core).
Axes of the slice: x: 8, y: 8, z: 8, core: 2. Of those that a mesh axis runs over, the one named last changes fastest.
Arguments:
- normed_input: bfloat16 [64, 128, 4096], P('exp', None, 'head'), may hold values from -11 to 11
- norm_gain: float32 [4096], P('head'), may hold values from 0.5 to 1.5
- norm_scale: float32 [64, 128], P('exp'), may hold values from 0.4 to 4
- out_grad: bfloat16 [64, 128, 4096], P('exp', None, 'head'), may hold values from -6 to 6
- router_weight: bfloat16 [4096, 128], P('head'), may hold values from -0.125 to 0.125
- routed_experts: int32 [64, 128, 8], P('exp'), may hold values from 0 to 127, all different within a row; in each aligned block of 128 rows (0 to 127, 128 to 255, ..., all dimensions but the last counted through in order) at most 15 rows name the same one
- expert_grad: bfloat16 [128, 64, 15, 4096], P('exp', None, None, 'head'), may hold values from -10 to 10, as said below
- gate_grad: bfloat16 [128, 64, 15], P('exp'), may hold values from -48 to 48
- out_proj: bfloat16 [8192, 4096], P('head'), may hold values from -0.0625 to 0.0625
- query_states: bfloat16 [64, 128, 8192], P('exp', None, 'head'), may hold values from -5 to 5
- rotated_keys: bfloat16 [64, 128, 512], P('exp'), may hold values from -5 to 5
- value_tensor: bfloat16 [64, 128, 512], P('exp'), may hold values from -6 to 6
Outputs:
- grad_hidden: bfloat16 [64, 128, 4096], P('exp', None, 'head')
- grad_query: bfloat16 [64, 128, 8192], P('exp', 'head')
- key_gradient: bfloat16 [64, 128, 512], P('exp', 'head')
- value_gradient: bfloat16 [64, 128, 512], P('exp', 'head')
The draws below stay inside these ranges and needn't reach their ends.
Inputs may be any that keep to these rules, and one draw needn't show every extreme that they name: `routed_experts`: each token names 8 different experts. Within one sequence, an aligned block of 128 rows, no expert is named by more than 15 tokens, a bound that some block reaches. `expert_grad`: slot c of expert e for sequence s holds the row of the c-th token of sequence s, in order of position, that names e; slots past that count hold unrelated values. `gate_grad`: same slot layout as expert_grad.
All inputs are finite; a program needn't handle non-finite values.
Results may differ from the reference program's by a relative error of at most 0.01225.
Values may be sent and summed in bfloat16 or wider, within the bound.
No kernel may reach another device: no remote copies, remote signals or barrier semaphores. Data moves between devices by JAX's collectives and lax.ppermute only.
A program may use at most 32 MiB of HBM per device.

```python
import math
import jax
import jax.numpy as jnp
import numpy as np
from jax import lax

D = 4096
QUERY_HEADS = 64
KEY_VALUE_HEADS = 4
HEAD_WIDTH = 128
TOPK = 8
EXPERTS = 128
SEQUENCE_COUNT = 64
SEQUENCE_TOKENS = 128
CAP = 15
N_HEAD = 16


def shared_rows(key):
    random_subkeys = jax.random.split(jax.random.fold_in(key, 101), 6)
    column_ramp = 0.5 + 1.5 * jnp.arange(D, dtype=jnp.float32) / D
    common = jnp.clip(jax.random.normal(random_subkeys[0], (D,), jnp.float32), -3.0, 3.0) * column_ramp
    return (random_subkeys, common)


def draw_normed_input(key, part):
    random_subkeys, common = shared_rows(key)
    base_rows = jnp.clip(jax.random.normal(random_subkeys[1], (SEQUENCE_COUNT, SEQUENCE_TOKENS, D), jnp.float32), -4.0, 4.0)
    drawn_rows = base_rows + 0.8 * common
    return drawn_rows.astype(jnp.bfloat16)


def draw_router_weight(key, part):
    random_subkeys, common = shared_rows(key)
    noise_part = jnp.clip(jax.random.normal(random_subkeys[3], (D, EXPERTS), jnp.float32), -4.0, 4.0)
    drawn_rows = noise_part * D ** (-0.5)
    return drawn_rows.astype(jnp.bfloat16)


def draw_expert_grad(key, part):
    random_subkeys, common = shared_rows(key)
    noise_part = jnp.clip(jax.random.normal(random_subkeys[5], (EXPERTS, SEQUENCE_COUNT, CAP, D), jnp.float32), -4.0, 4.0)
    drawn_rows = noise_part + 0.6 * common
    return drawn_rows.astype(jnp.bfloat16)


def attention_pair(key):
    random_subkeys = jax.random.split(jax.random.fold_in(key, 202), 2)
    queries = jnp.clip(jax.random.normal(random_subkeys[0], (SEQUENCE_COUNT, SEQUENCE_TOKENS, QUERY_HEADS * HEAD_WIDTH), jnp.float32), -4.0, 4.0)
    random_keyset = jnp.clip(jax.random.normal(random_subkeys[1], (SEQUENCE_COUNT, SEQUENCE_TOKENS, KEY_VALUE_HEADS * HEAD_WIDTH), jnp.float32), -4.0, 4.0)
    return (queries, random_keyset)


def draw_query_states(key, part):
    queries, random_keyset = attention_pair(key)
    return queries.astype(jnp.bfloat16)


def draw_rotated_keys(key, part):
    queries, random_keyset = attention_pair(key)
    return random_keyset.astype(jnp.bfloat16)


def steps_of(own_key, shape, cuts, smallest, largest):
    def one(dim, blocks):
        heights = jax.random.uniform(jax.random.fold_in(jax.random.fold_in(own_key, 6), dim), (blocks,), jnp.float32, smallest / len(cuts), largest / len(cuts))
        return jnp.repeat(jnp.exp(heights), shape[dim] // blocks).reshape((-1,) + (1,) * (len(shape) - dim - 1))

    factor_of = one(*cuts[0])
    for cut in cuts[1:]:
        factor_of = factor_of * one(*cut)
    return factor_of


def shared_out(own_key, own, number, rows, number_of, top, limit, slope):
    order = jax.random.permutation(own_key, number_of)
    crowded, ordinary = portions_of(number_of, rows * top, limit, slope, True), portions_of(number_of, rows * top, limit, slope, False)
    places = jnp.arange(number_of)

    def named(sizes, turn):
        used = int((sizes > 0).sum())
        fixed = max(1, used // 4)
        moved = fixed + (places - fixed + turn * (used - fixed)) % max(1, number_of - fixed)
        return jnp.zeros((number_of,), jnp.int32).at[order[jnp.where(places < fixed, places, moved)]].set(jnp.asarray(sizes, jnp.int32))

    sizes = jnp.where(number % 4 == 0, named(crowded, number // 4), named(ordinary, number - number // 4 - 1))
    mixed = jax.random.permutation(jax.random.fold_in(own, 3), number_of)
    source_of, taker = mixed[0:number_of // 2 * 2:2], mixed[1:number_of // 2 * 2:2]
    margin = jnp.minimum(sizes[source_of] - 1, limit - sizes[taker]) // 2
    margin = jnp.where((source_of == order[0]) | (taker == order[0]) | (sizes[taker] == 0), 0, jnp.maximum(margin, 0))
    moved = jax.random.randint(jax.random.fold_in(own, 4), (number_of // 2,), 0, 1 << 20) % (margin + 1)
    sizes = sizes.at[source_of].add(-moved).at[taker].add(moved)
    labels = jnp.searchsorted(jnp.cumsum(sizes), jnp.arange(rows * top), side="right").astype(jnp.int32)
    listing = labels.reshape(top, rows).T
    listing = listing[jax.random.permutation(jax.random.fold_in(own, 1), rows)]
    turn = jax.random.randint(jax.random.fold_in(own, 2), (rows, 1), 0, top)
    return jnp.take_along_axis(listing, (jnp.arange(top)[None, :] + turn) % top, axis=1)


def portions_of(count, total, most, skew, full):
    weights = [(1 << 20) // math.isqrt(rank ** skew) + 1 for rank in range(1, count + 1)]
    largest = most if full else min(most, max(-(-total // count), total * weights[0] // sum(weights)))
    least = 1 if total - largest >= count - 1 else 0
    counts, spare = [largest] + [least] * (count - 1), total - largest - least * (count - 1)
    while spare > 0:
        candidates = [i for i in range(1, count) if counts[i] < largest] or [i for i in range(1, count) if counts[i] < most]
        pool, left = sum([weights[i] for i in candidates]), spare
        for i in candidates:
            addition = min(most - counts[i], max(1, left * weights[i] // pool), spare)
            counts[i] = counts[i] + addition
            spare = spare - addition
    return np.array(counts)


def bell_draw(key, shape, scale, reach, pieces=(), held_as=jnp.bfloat16):
    entries = scale * jax.random.normal(key, shape, jnp.float32)
    if pieces:
        entries = entries * steps_of(key, shape, pieces, -0.22, 0.18)
    return jnp.clip(entries, -reach, reach).astype(held_as)


def setup_inputs(seed: int = 0) -> dict:
    splits = jax.random.split(jax.random.key(seed), 13)
    normed_input = draw_normed_input(jax.random.fold_in(splits[12], 71), 0)
    norm_gain = jnp.clip(1.0 + 0.1 * jax.random.normal(splits[1], (D,), jnp.float32), 0.5, 1.5)
    norm_scale = jnp.clip(jnp.exp(math.log(4.0) - 2.3025851 * jax.random.uniform(splits[2], (SEQUENCE_COUNT, SEQUENCE_TOKENS), jnp.float32) ** steps_of(splits[2], (SEQUENCE_COUNT, SEQUENCE_TOKENS), ((0, 64),), -0.2, 0.2)), 0.4, 4.0)
    out_grad = bell_draw(splits[3], (SEQUENCE_COUNT, SEQUENCE_TOKENS, D), 1.0, 6.0, ((0, 64), (2, 16)))
    router_weight = draw_router_weight(jax.random.fold_in(splits[12], 71), 0)
    routed_experts_keys = jax.random.split(jax.random.fold_in(splits[5], 1), SEQUENCE_COUNT * SEQUENCE_TOKENS // SEQUENCE_TOKENS)
    routed_experts_turns = jax.random.permutation(jax.random.fold_in(splits[5], 3), SEQUENCE_COUNT * SEQUENCE_TOKENS // SEQUENCE_TOKENS)
    routed_experts = jax.vmap(lambda own, number: shared_out(jax.random.fold_in(splits[5], 2), own, number, SEQUENCE_TOKENS, EXPERTS, TOPK, CAP, 2))(routed_experts_keys, routed_experts_turns).reshape((SEQUENCE_COUNT, SEQUENCE_TOKENS, TOPK))
    expert_grad = draw_expert_grad(jax.random.fold_in(splits[12], 71), 0)
    gate_grad = bell_draw(splits[7], (EXPERTS, SEQUENCE_COUNT, CAP), 8.0, 48.0, ((0, 64),))
    out_proj = bell_draw(splits[8], (QUERY_HEADS * HEAD_WIDTH, D), (QUERY_HEADS * HEAD_WIDTH) ** -0.5, 0.0625, ((0, 16),))
    query_states = draw_query_states(jax.random.fold_in(splits[12], 71), 0)
    rotated_keys = draw_rotated_keys(jax.random.fold_in(splits[12], 71), 0)
    value_tensor = bell_draw(splits[11], (SEQUENCE_COUNT, SEQUENCE_TOKENS, KEY_VALUE_HEADS * HEAD_WIDTH), 1.0, 6.0, ((0, 64),))
    return dict(normed_input=normed_input, norm_gain=norm_gain, norm_scale=norm_scale, out_grad=out_grad, router_weight=router_weight, routed_experts=routed_experts, expert_grad=expert_grad, gate_grad=gate_grad, out_proj=out_proj, query_states=query_states, rotated_keys=rotated_keys, value_tensor=value_tensor)


def reference(normed_input, norm_gain, norm_scale, out_grad, router_weight, routed_experts, expert_grad, gate_grad, out_proj, query_states, rotated_keys, value_tensor):
    highest = lax.Precision.HIGHEST
    expert_iota = lax.iota(jnp.int32, EXPERTS)
    weight_full = router_weight.astype(jnp.float32)
    group_width = QUERY_HEADS // KEY_VALUE_HEADS
    resident_heads = QUERY_HEADS // N_HEAD
    replica_count = N_HEAD // KEY_VALUE_HEADS

    def per_sequence(sequence_index):
        hidden_part = normed_input[sequence_index].astype(jnp.float32)
        expert_ids = routed_experts[sequence_index].astype(jnp.int32)
        slot_table = expert_grad[:, sequence_index].reshape(EXPERTS * CAP, D)
        gate_table = gate_grad[:, sequence_index].reshape(EXPERTS * CAP)
        scaled = hidden_part * norm_gain
        normed = scaled.astype(jnp.bfloat16)
        logits = jnp.dot(normed, router_weight, preferred_element_type=jnp.float32)
        picked = jnp.take_along_axis(logits, expert_ids, axis=1)
        gate_weights = jax.nn.softmax(picked, axis=-1)
        member = expert_ids[:, :, None] == expert_iota[None, None, :]
        per_token = lax.optimization_barrier(jnp.sum(member.astype(jnp.int32), axis=1, dtype=jnp.int32))
        before = jnp.cumsum(per_token, axis=0, dtype=jnp.int32) - per_token
        slot_index = lax.optimization_barrier(jnp.sum(jnp.where(member, before[:, None, :], 0), axis=-1, dtype=jnp.int32))
        flat_index = (expert_ids * CAP + slot_index).astype(jnp.int32)
        slot_rows = jnp.take(slot_table, flat_index, axis=0).astype(jnp.float32)
        slot_grads = jnp.take(gate_table, flat_index).astype(jnp.float32)
        gate_diff = gate_weights * (slot_grads - lax.optimization_barrier(jnp.sum(gate_weights * slot_grads, axis=-1, keepdims=True)))
        diff_full = jnp.einsum('lk,lke->le', gate_diff, member.astype(jnp.float32), precision=highest)
        grad_normed = jnp.einsum('lk,lkd->ld', gate_weights, slot_rows, precision=highest)
        grad_normed = grad_normed + jnp.dot(diff_full, weight_full.T, precision=highest)
        inner = lax.optimization_barrier(jnp.sum(scaled * grad_normed, axis=-1))
        grad_hidden = out_grad[sequence_index].astype(jnp.float32) + norm_scale[sequence_index][:, None] * (norm_gain * grad_normed - hidden_part * inner[:, None] / D)
        grad_hidden = grad_hidden.astype(jnp.bfloat16)
        context_grad = jnp.dot(grad_hidden, out_proj.T, preferred_element_type=jnp.float32).astype(jnp.bfloat16)
        queries = query_states[sequence_index].reshape(SEQUENCE_TOKENS, QUERY_HEADS, HEAD_WIDTH).astype(jnp.float32)
        key_row_block = jnp.repeat(rotated_keys[sequence_index].reshape(SEQUENCE_TOKENS, KEY_VALUE_HEADS, HEAD_WIDTH), group_width, axis=1).astype(jnp.float32)
        value_row_block = jnp.repeat(value_tensor[sequence_index].reshape(SEQUENCE_TOKENS, KEY_VALUE_HEADS, HEAD_WIDTH), group_width, axis=1).astype(jnp.float32)
        grads_ctx = context_grad.reshape(SEQUENCE_TOKENS, QUERY_HEADS, HEAD_WIDTH).astype(jnp.float32)
        root = jnp.sqrt(jnp.float32(HEAD_WIDTH))
        scores = jnp.einsum('qhd,khd->hqk', queries, key_row_block) / root
        positions = lax.iota(jnp.int32, SEQUENCE_TOKENS)
        causal = positions[:, None] >= positions[None, :]
        scores = jnp.where(causal[None], scores, -jnp.inf)
        attn_probs = jax.nn.softmax(scores, axis=-1)
        probs_low = attn_probs.astype(jnp.bfloat16)
        prob_grads = jnp.einsum('qhd,khd->hqk', grads_ctx, value_row_block)
        row_delta = lax.optimization_barrier(jnp.sum(attn_probs * prob_grads, axis=-1, keepdims=True))
        score_grads = (attn_probs * (prob_grads - row_delta) / root).astype(jnp.bfloat16)
        score_f = score_grads.astype(jnp.float32)
        grad_query = jnp.einsum('hqk,khd->qhd', score_f, key_row_block).astype(jnp.bfloat16).reshape(SEQUENCE_TOKENS, QUERY_HEADS * HEAD_WIDTH)
        key_heads = jnp.einsum('hqk,qhd->hkd', score_f, queries)
        value_heads = jnp.einsum('hqk,qhd->hkd', probs_low.astype(jnp.float32), grads_ctx)
        partial_key_sum = lax.optimization_barrier(jnp.sum(key_heads.reshape(N_HEAD, resident_heads, SEQUENCE_TOKENS, HEAD_WIDTH), axis=1)).astype(jnp.bfloat16)
        partial_value_sum = lax.optimization_barrier(jnp.sum(value_heads.reshape(N_HEAD, resident_heads, SEQUENCE_TOKENS, HEAD_WIDTH), axis=1)).astype(jnp.bfloat16)
        key_gradient = lax.optimization_barrier(jnp.sum(partial_key_sum.astype(jnp.float32).reshape(KEY_VALUE_HEADS, replica_count, SEQUENCE_TOKENS, HEAD_WIDTH), axis=1)).astype(jnp.bfloat16)
        value_gradient = lax.optimization_barrier(jnp.sum(partial_value_sum.astype(jnp.float32).reshape(KEY_VALUE_HEADS, replica_count, SEQUENCE_TOKENS, HEAD_WIDTH), axis=1)).astype(jnp.bfloat16)
        key_gradient = jnp.transpose(key_gradient, (1, 0, 2)).reshape(SEQUENCE_TOKENS, KEY_VALUE_HEADS * HEAD_WIDTH)
        value_gradient = jnp.transpose(value_gradient, (1, 0, 2)).reshape(SEQUENCE_TOKENS, KEY_VALUE_HEADS * HEAD_WIDTH)
        return (grad_hidden, grad_query, key_gradient, value_gradient)
    results = lax.map(per_sequence, jnp.arange(SEQUENCE_COUNT, dtype=jnp.int32))
    return (results[0], results[1], results[2], results[3])
```

```python
import math

import jax
import jax.numpy as jnp
from jax import lax
from jax.experimental import pallas as pl
from jax.experimental.pallas import tpu as pltpu
from jax.sharding import PartitionSpec as P


HEAD_WIDTH = 128
KEY_VALUE_HEADS = 4
TOPK = 8
F32 = jnp.float32
BF16 = jnp.bfloat16
TOKENS = 128
SLOTS = 16
ROWS = 144
TAIL = 136
GRANT = 24 * 2**20


def call(kernel, outs, *args):
    specs = [pl.BlockSpec(memory_space=pltpu.SMEM) if a.dtype == jnp.int32 and a.size == 1
             else pl.BlockSpec(memory_space=pltpu.VMEM) for a in args]
    one = isinstance(outs, jax.ShapeDtypeStruct)
    vm = pl.BlockSpec(memory_space=pltpu.VMEM)
    return pl.pallas_call(
        kernel,
        out_shape=outs,
        in_specs=specs,
        out_specs=vm if one else tuple(vm for _ in outs),
        compiler_params=pltpu.CompilerParams(vmem_limit_bytes=GRANT),
    )(*args)


def shape(s, d=F32):
    return jax.ShapeDtypeStruct(s, d)


def nn(a, b):
    return lax.dot_general(a, b, (((1,), (0,)), ((), ())), preferred_element_type=F32)


def nt(a, b):
    return lax.dot_general(a, b, (((1,), (1,)), ((), ())), preferred_element_type=F32)


def high_low(v):
    high = v.astype(BF16)
    return high, (v - high.astype(F32)).astype(BF16)


def three(v):
    a = v.astype(BF16)
    rest = v - a.astype(F32)
    b = rest.astype(BF16)
    return a, b, (rest - b.astype(F32)).astype(BF16)


def logits_kernel(x, gain, router, ids, sent):
    xv = x[...]
    scaled = xv.astype(F32) * gain[...]
    logits = nn(scaled.astype(BF16), router[...]).T
    experts = lax.broadcasted_iota(jnp.int32, logits.shape, 0)
    rows = []
    for k in range(TOPK):
        rows.append(jnp.sum(jnp.where(ids[k : k + 1, :] == experts, logits, 0.0), axis=0, keepdims=True))
    a, b, c = three(jnp.concatenate(rows, axis=0))
    sent[0:TOKENS, :] = xv
    sent[TOKENS : TOKENS + 8, 0:128] = a
    sent[TOKENS : TOKENS + 8, 128:256] = b
    sent[TOKENS + 8 : ROWS, 0:128] = c
    sent[TOKENS + 8 : ROWS, 128:256] = jnp.zeros_like(c)


def picks_kernel(own, total_out):
    total = jnp.zeros((8, 128), F32)
    for i in range(own.shape[0]):
        top = own[i, TOKENS : TOKENS + 8, :].astype(F32)
        low = own[i, TOKENS + 8 : ROWS, 0:128].astype(F32)
        total = total + ((top[:, 0:128] + top[:, 128:256]) + low)
    total_out[...] = total


def weights_kernel(own, other, ids, mix, dense, rank):
    total = own[...] + other[...]
    top = jnp.max(total, axis=0, keepdims=True)
    e = jnp.exp(total - top)
    gates = e / jnp.sum(e, axis=0, keepdims=True)
    n = dense.shape[0]
    experts = lax.broadcasted_iota(jnp.int32, (n, TOKENS), 0)
    weight = jnp.zeros((n, TOKENS), F32)
    member = jnp.zeros((n, TOKENS), F32)
    for k in range(TOPK):
        hit = ids[k : k + 1, :] == experts
        weight = jnp.where(hit, gates[k : k + 1, :], weight)
        member = jnp.where(hit, 1.0, member)
    t_from = lax.broadcasted_iota(jnp.int32, (TOKENS, TOKENS), 0)
    t_to = lax.broadcasted_iota(jnp.int32, (TOKENS, TOKENS), 1)
    earlier = jnp.where(t_from < t_to, 1.0, 0.0).astype(BF16)
    before = nn(member.astype(BF16), earlier)
    dense[...] = weight
    rank[...] = before
    step = 8
    for g in range(n // step):
        w3 = weight[g * step : (g + 1) * step, :][:, None, :]
        b3 = before[g * step : (g + 1) * step, :][:, None, :]
        slot = lax.broadcasted_iota(jnp.int32, (step, SLOTS, TOKENS), 1).astype(F32)
        block = jnp.where(jnp.broadcast_to(b3, slot.shape) == slot, jnp.broadcast_to(w3, slot.shape), 0.0)
        block = block.reshape(step * SLOTS, TOKENS).T
        mix[:, g * step * SLOTS : (g + 1) * step * SLOTS] = block.astype(BF16)


def rows_kernel(received, mix, dense, rank, router, x, gain, scale, out_grad, sent, full):
    n = dense.shape[0]
    rows = received[...]
    both = nn(mix[...], rows)
    e_of = lax.broadcasted_iota(jnp.int32, (n, n * SLOTS), 0)
    j_of = lax.broadcasted_iota(jnp.int32, (n, n * SLOTS), 1)
    pick = jnp.where(j_of == e_of * SLOTS + (SLOTS - 1), 1.0, 0.0).astype(BF16)
    table = nn(pick, received[:, 0:128])
    ranks = rank[...]
    slot_grads = jnp.zeros((n, TOKENS), F32)
    for c in range(SLOTS - 1):
        slot_grads = jnp.where(ranks == float(c), table[:, c : c + 1], slot_grads)
    weight = dense[...]
    mean = jnp.sum(weight * slot_grads, axis=0, keepdims=True)
    diff = (weight * (slot_grads - mean)).T
    d_high, d_low = high_low(diff)
    routed = nt(d_high, router[...]) + nt(d_low, router[...])
    grad = both + routed
    inner_terms = x[...].astype(F32) * gain[...] * grad
    i_high, i_mid, i_low = three(inner_terms)
    ones = jnp.ones((8, 256), BF16)
    inner = (nt(ones, i_high) + nt(ones, i_mid)) + nt(ones, i_low)
    s = jnp.broadcast_to(scale[...], (TOKENS, TOKENS)).T
    moved = out_grad[...].astype(F32) + jnp.concatenate([s, s], axis=1) * (gain[...] * grad)
    full[...] = moved
    low = moved.astype(BF16)
    a, b, c = three(inner)
    row = lax.broadcasted_iota(jnp.int32, (8, 256), 0)
    first = jnp.concatenate([a.astype(F32), b.astype(F32)], axis=1)
    second = jnp.concatenate([c.astype(F32), jnp.zeros((8, 128), F32)], axis=1)
    extra = jnp.where(row == 0, first, jnp.where(row == 1, second, 0.0)).astype(BF16)
    for i in range(sent.shape[0]):
        sent[i, 0:TOKENS, :] = low
        sent[i, TOKENS:TAIL, :] = extra


def contract(part, proj, core):
    total = None
    for i in range(part.shape[0]):
        at = pl.multiple_of(i * 512 + core * 256, 256)
        term = nt(part[i, 0:TOKENS, :], proj[:, pl.ds(at, 256)])
        total = term if total is None else total + term
    return total


def half_kernel(place, own, proj, out):
    out[...] = contract(own, proj, place[0] % 2)


def early_kernel(place, own, other, proj, queries, keys, hidden_ctx, probs):
    core = place[0] % 2
    hidden_ctx[...] = contract(own, proj, core) + contract(other, proj, 1 - core)
    inv_sqrt = 1.0 / math.sqrt(HEAD_WIDTH)
    kv = pl.multiple_of(place[0] // KEY_VALUE_HEADS * HEAD_WIDTH, HEAD_WIDTH)
    key = keys[:, pl.ds(kv, HEAD_WIDTH)]
    at_key = lax.broadcasted_iota(jnp.int32, (TOKENS, TOKENS), 0)
    at_query = lax.broadcasted_iota(jnp.int32, (TOKENS, TOKENS), 1)
    for h in range(probs.shape[0]):
        scores = nt(key, queries[:, h * 128 : (h + 1) * 128]) * inv_sqrt
        scores = jnp.where(at_key <= at_query, scores, -jnp.inf)
        e = jnp.exp(scores - jnp.max(scores, axis=0, keepdims=True))
        probs[h] = e / jnp.sum(e, axis=0, keepdims=True)


def attention_kernel(place, own, other, half, proj, queries, keys, values, hidden_ctx, probs, scale, width, sent, shift):
    core = place[0] % 2
    row = jnp.zeros((1, 128), F32)
    for part in (own, other):
        for i in range(part.shape[0]):
            tail = part[i, TOKENS:TAIL, :].astype(F32)
            row = row + ((tail[0:1, 0:128] + tail[0:1, 128:256]) + tail[1:2, 0:128])
    column = jnp.broadcast_to(row * scale[...] / width[0].astype(F32), (TOKENS, TOKENS)).T
    shift[...] = column
    inv_sqrt = 1.0 / math.sqrt(HEAD_WIDTH)
    kv = pl.multiple_of(place[0] // KEY_VALUE_HEADS * HEAD_WIDTH, HEAD_WIDTH)
    key = keys[:, pl.ds(kv, HEAD_WIDTH)]
    value = values[:, pl.ds(kv, HEAD_WIDTH)]
    ctx = half[...] + contract(other, proj, 1 - core)
    n = probs.shape[0]
    key_sum = jnp.zeros((TOKENS, HEAD_WIDTH), F32)
    value_sum = jnp.zeros((TOKENS, HEAD_WIDTH), F32)
    for h in range(n):
        cols = slice(h * 128, (h + 1) * 128)
        grads = (ctx[:, cols] - column * hidden_ctx[:, cols]).astype(BF16)
        p = probs[h]
        prob_grads = nt(value, grads)
        delta = jnp.sum(p * prob_grads, axis=0, keepdims=True)
        score_grads = p * (prob_grads - delta) * inv_sqrt
        low = score_grads.astype(BF16)
        sent[:, cols] = nn(score_grads.T.astype(BF16), key).astype(BF16)
        key_sum = key_sum + nn(low, queries[:, cols])
        value_sum = value_sum + nn(p.astype(BF16), grads)
    sent[:, n * 128 : n * 128 + 128] = key_sum.astype(BF16)
    sent[:, n * 128 + 128 : n * 128 + 256] = value_sum.astype(BF16)


def hidden_kernel(full, x, shift, out):
    s = shift[...]
    out[...] = (full[...] - x[...].astype(F32) * jnp.concatenate([s, s], axis=1)).astype(BF16)


def collect_kernel(received, query_out, key_out, value_out):
    n = received.shape[0]
    heads = received.shape[2] - 256
    for i in range(n):
        query_out[:, i * heads : (i + 1) * heads] = received[i, :, 0:heads]
    group = n // KEY_VALUE_HEADS
    for g in range(KEY_VALUE_HEADS):
        for out, at in ((key_out, heads), (value_out, heads + 128)):
            parts = [received[g * group + r, :, at : at + 128].astype(F32) for r in range(group)]
            total = parts[0]
            for part in parts[1:]:
                total = total + part
            out[:, g * 128 : (g + 1) * 128] = total.astype(BF16)


def per_device(
    normed_input,
    norm_gain,
    norm_scale,
    out_grad,
    router_weight,
    routed_experts,
    expert_grad,
    gate_grad,
    out_proj,
    query_states,
    rotated_keys,
    value_tensor,
):
    held, sequences, capacity, columns = expert_grad.shape
    n_head = lax.axis_size("head")
    n_experts = router_weight.shape[1]
    cores = [[2 * i + c for i in range(n_head // 2)] for c in range(2)]
    swap = [(i, i ^ 1) for i in range(n_head)]
    place = lax.axis_index("head").reshape(1)
    x, ids = normed_input[0], routed_experts[0].T
    gain = norm_gain.reshape(1, columns)
    width = jnp.full((1,), out_proj.shape[1], jnp.int32)

    local = out_proj.shape[0]
    gates = jnp.pad(gate_grad.transpose(1, 0, 2)[:, :, None, :], ((0, 0), (0, 0), (0, 0), (0, columns - capacity)))
    packed = jnp.concatenate([expert_grad.transpose(1, 0, 2, 3), gates], axis=2)
    packed = packed.reshape(sequences, held * SLOTS, columns)
    received = lax.all_to_all(packed, "exp", split_axis=0, concat_axis=0, tiled=True)
    received = received.reshape(n_experts * SLOTS, columns)
    early = call(logits_kernel, shape((ROWS, columns), BF16), x, gain, router_weight, ids)
    early_own = lax.all_gather(early, "head", axis_index_groups=cores)
    picks = call(picks_kernel, shape((8, 128)), early_own)
    picks_other = lax.ppermute(picks, "head", swap)
    mix, dense, rank = call(
        weights_kernel,
        (shape((TOKENS, n_experts * SLOTS), BF16), shape((n_experts, TOKENS)), shape((n_experts, TOKENS))),
        picks, picks_other, ids,
    )
    late, full = call(
        rows_kernel,
        (shape((n_head // 2, TAIL, columns), BF16), shape((TOKENS, columns))),
        received, mix, dense, rank, router_weight, x, gain, norm_scale, out_grad[0],
    )
    late_own = lax.all_to_all(late, "head", split_axis=0, concat_axis=0, tiled=True, axis_index_groups=cores)
    early_other = lax.ppermute(early_own, "head", swap)
    hidden_ctx, probs = call(
        early_kernel,
        (shape((TOKENS, local)), shape((local // HEAD_WIDTH, TOKENS, TOKENS))),
        place, early_own, early_other, out_proj, query_states[0], rotated_keys[0],
    )
    late_other = lax.ppermute(late_own, "head", swap)
    half = call(half_kernel, shape((TOKENS, local)), place, late_own, out_proj)
    grads, shift = call(
        attention_kernel,
        (shape((TOKENS, local + 256), BF16), shape((TOKENS, TOKENS))),
        place, late_own, late_other, half, out_proj, query_states[0], rotated_keys[0], value_tensor[0],
        hidden_ctx, probs, norm_scale, width,
    )
    grad_hidden = call(hidden_kernel, shape((TOKENS, columns), BF16), full, x, shift)
    tokens = TOKENS // n_head
    returned = lax.all_to_all(
        grads.reshape(n_head, tokens, local + 256), "head", split_axis=0, concat_axis=0, tiled=True
    )
    query_out, key_out, value_out = call(
        collect_kernel,
        (shape((tokens, n_head * local), BF16), shape((tokens, 512), BF16), shape((tokens, 512), BF16)),
        returned,
    )
    return (grad_hidden[None], query_out[None], key_out[None], value_out[None])


def solution(mesh):
    placed = (
        P("exp", None, "head"),
        P("head"),
        P("exp", None),
        P("exp", None, "head"),
        P("head", None),
        P("exp", None, None),
        P("exp", None, None, "head"),
        P("exp", None, None),
        P("head", None),
        P("exp", None, "head"),
        P("exp", None, None),
        P("exp", None, None),
    )
    return jax.shard_map(
        per_device,
        mesh=mesh,
        in_specs=placed,
        out_specs=(
            P("exp", None, "head"),
            P("exp", "head", None),
            P("exp", "head", None),
            P("exp", "head", None),
        ),
        check_vma=False,
    )
```

```python
import math

import jax
import jax.numpy as jnp
from jax import lax
from jax.experimental import pallas as pl
from jax.experimental.pallas import tpu as pltpu
from jax.sharding import PartitionSpec as P


HEAD_WIDTH = 128
KEY_VALUE_HEADS = 4
TOPK = 8
F32 = jnp.float32
BF16 = jnp.bfloat16
TOKENS = 128
SLOTS = 16
MAIN = 112
LEFT = TOKENS - MAIN
ROWS = MAIN + 8
GRANT = 24 * 2**20


def call(kernel, outs, *args, far=(), far_out=False, scratch=()):
    specs = [
        pl.BlockSpec(
            memory_space=pltpu.SMEM if a.dtype == jnp.int32 and a.size == 1 else pltpu.HBM if i in far else pltpu.VMEM
        )
        for i, a in enumerate(args)
    ]
    args = [pltpu.with_memory_space_constraint(a, pltpu.HBM) if i in far else a for i, a in enumerate(args)]
    one = isinstance(outs, jax.ShapeDtypeStruct)
    vm, hbm = pl.BlockSpec(memory_space=pltpu.VMEM), pl.BlockSpec(memory_space=pltpu.HBM)
    return pl.pallas_call(
        kernel,
        out_shape=outs,
        in_specs=specs,
        out_specs=vm if one else tuple(hbm if far_out else vm for _ in outs),
        scratch_shapes=scratch,
        compiler_params=pltpu.CompilerParams(vmem_limit_bytes=GRANT),
    )(*args)


def shape(s, d=F32):
    return jax.ShapeDtypeStruct(s, d)


def nn(a, b):
    return lax.dot_general(a, b, (((1,), (0,)), ((), ())), preferred_element_type=F32)


def nt(a, b):
    return lax.dot_general(a, b, (((1,), (1,)), ((), ())), preferred_element_type=F32)


def high_low(v):
    high = v.astype(BF16)
    return high, (v - high.astype(F32)).astype(BF16)


def three(v):
    a = v.astype(BF16)
    rest = v - a.astype(F32)
    b = rest.astype(BF16)
    return a, b, (rest - b.astype(F32)).astype(BF16)


def pack_kernel(rows, gates, out, table):
    held, capacity, chunk, columns = rows.shape

    @pl.when(pl.program_id(0) == 0)
    def _():
        flat = gates[...].astype(F32)
        n = flat.shape[2]
        for e in range(held):
            wide = jnp.concatenate([flat[:, e, :], jnp.zeros((capacity, 128 - n), F32)], axis=1)
            table[e] = jnp.concatenate([wide, jnp.zeros((128 - capacity, 128), F32)], axis=0).T[0:n]

    at = pl.multiple_of(pl.program_id(0) * chunk, chunk)
    for e in range(held):
        for lane in range(0, columns, 128):
            last = table[e, pl.ds(at, chunk), :] if lane == 0 else jnp.zeros((chunk, 128), F32)
            block = jnp.concatenate([rows[e, :, :, lane : lane + 128].astype(F32), last[None]], axis=0)
            out[:, e * SLOTS : (e + 1) * SLOTS, lane : lane + 128] = jnp.swapaxes(block, 0, 1).astype(BF16)


def pack(expert_grad, gate_grad):
    held, n, capacity, columns = expert_grad.shape
    chunk = min(n, 16)
    run = pl.pallas_call(
        pack_kernel,
        grid=(n // chunk,),
        in_specs=[
            pl.BlockSpec((held, capacity, chunk, columns), lambda i: (0, 0, i, 0)),
            pl.BlockSpec((capacity, held, n), lambda i: (0, 0, 0)),
        ],
        out_specs=pl.BlockSpec((chunk, held * SLOTS, columns), lambda i: (i, 0, 0)),
        out_shape=shape((n, held * SLOTS, columns), BF16),
        scratch_shapes=[pltpu.VMEM((held, n, 128), F32)],
        name="pack",
        compiler_params=pltpu.CompilerParams(vmem_limit_bytes=GRANT),
    )
    stay = lambda a: pltpu.with_memory_space_constraint(a, pltpu.HBM)
    return run(stay(expert_grad.transpose(0, 2, 1, 3)), stay(gate_grad.transpose(2, 0, 1)))


def logits_kernel(x, gain, router, ids, sent):
    xv = x[...]
    scaled = xv.astype(F32) * gain[...]
    logits = nn(scaled.astype(BF16), router[...]).T
    experts = lax.broadcasted_iota(jnp.int32, logits.shape, 0)
    rows = []
    for k in range(TOPK):
        rows.append(jnp.sum(jnp.where(ids[k : k + 1, :] == experts, logits, 0.0), axis=0, keepdims=True))
    a, b = high_low(jnp.concatenate(rows, axis=0))
    sent[0:MAIN, :] = xv[0:MAIN]
    sent[MAIN:ROWS, 0:128] = a
    sent[MAIN:ROWS, 128:256] = b


def spread(gates, ids):
    n = gates.shape[1]
    experts = lax.broadcasted_iota(jnp.int32, (n, TOKENS), 0)
    weight = jnp.zeros((n, TOKENS), F32)
    member = jnp.zeros((n, TOKENS), F32)
    for k in range(TOPK):
        hit = ids[k : k + 1, :] == experts
        weight = jnp.where(hit, gates[k : k + 1, :], weight)
        member = jnp.where(hit, 1.0, member)
    t_from = lax.broadcasted_iota(jnp.int32, (TOKENS, TOKENS), 0)
    t_to = lax.broadcasted_iota(jnp.int32, (TOKENS, TOKENS), 1)
    earlier = jnp.where(t_from < t_to, 1.0, 0.0).astype(BF16)
    return weight, nn(member.astype(BF16), earlier)


def weights_kernel(gathered, ids, mix, gates_out):
    total = jnp.zeros((8, 128), F32)
    for i in range(gathered.shape[0]):
        both = gathered[i, MAIN:ROWS, :].astype(F32)
        total = total + (both[:, 0:128] + both[:, 128:256])
    top = jnp.max(total, axis=0, keepdims=True)
    e = jnp.exp(total - top)
    gates = e / jnp.sum(e, axis=0, keepdims=True)
    gates_out[...] = gates
    weight, before = spread(gates, ids)
    step = 8
    for g in range(weight.shape[0] // step):
        w3 = weight[g * step : (g + 1) * step, :][:, None, :]
        b3 = before[g * step : (g + 1) * step, :][:, None, :]
        slot = lax.broadcasted_iota(jnp.int32, (step, SLOTS, TOKENS), 1).astype(F32)
        block = jnp.where(jnp.broadcast_to(b3, slot.shape) == slot, jnp.broadcast_to(w3, slot.shape), 0.0)
        block = block.reshape(step * SLOTS, TOKENS).T
        mix[:, g * step * SLOTS : (g + 1) * step * SLOTS] = block.astype(BF16)


def rows_kernel(received, mix, gates, ids, router, x, gain, scale, out_grad, sent_out, rest_out, full_out, sent, rest, full, done):
    weight, ranks = spread(gates[...], ids)
    n = weight.shape[0]
    rows = received[...]
    both = nn(mix[...], rows)
    e_of = lax.broadcasted_iota(jnp.int32, (n, n * SLOTS), 0)
    j_of = lax.broadcasted_iota(jnp.int32, (n, n * SLOTS), 1)
    pick = jnp.where(j_of == e_of * SLOTS + (SLOTS - 1), 1.0, 0.0).astype(BF16)
    table = nn(pick, received[:, 0:128])
    slot_grads = jnp.zeros((n, TOKENS), F32)
    for c in range(SLOTS - 1):
        slot_grads = jnp.where(ranks == float(c), table[:, c : c + 1], slot_grads)
    mean = jnp.sum(weight * slot_grads, axis=0, keepdims=True)
    diff = (weight * (slot_grads - mean)).T
    d_high, d_low = high_low(diff)
    routed = nt(d_high, router[...]) + nt(d_low, router[...])
    grad = both + routed
    s = jnp.broadcast_to(scale[...], (TOKENS, TOKENS)).T
    moved = out_grad[...].astype(F32) + jnp.concatenate([s, s], axis=1) * (gain[...] * grad)
    low = moved.astype(BF16)
    full[...] = moved
    sent[0:MAIN, :] = low[0:MAIN]
    rest[0:LEFT, :] = low[MAIN:TOKENS]
    rest[LEFT : 2 * LEFT, :] = x[MAIN:TOKENS, :]
    n_head = rest_out.shape[0]
    copies = [pltpu.make_async_copy(rest, rest_out.at[i], done.at[i]) for i in range(n_head)]
    copies.append(pltpu.make_async_copy(full, full_out, done.at[n_head]))
    copies.append(pltpu.make_async_copy(sent.at[0:MAIN], sent_out.at[0:MAIN], done.at[n_head + 1]))
    for copy in copies:
        copy.start()
    inner_terms = x[...].astype(F32) * gain[...] * grad
    i_high, i_mid, i_low = three(inner_terms)
    ones = jnp.ones((8, 256), BF16)
    inner = (nt(ones, i_high) + nt(ones, i_mid)) + nt(ones, i_low)
    a, b, c = three(inner)
    row = lax.broadcasted_iota(jnp.int32, (8, 256), 0)
    first = jnp.concatenate([a.astype(F32), b.astype(F32)], axis=1)
    second = jnp.concatenate([c.astype(F32), jnp.zeros((8, 128), F32)], axis=1)
    extra = jnp.where(row == 0, first, jnp.where(row == 1, second, 0.0)).astype(BF16)
    sent[MAIN:ROWS, :] = extra
    copies.append(pltpu.make_async_copy(sent.at[MAIN:ROWS], sent_out.at[MAIN:ROWS], done.at[n_head + 2]))
    copies[-1].start()
    for copy in copies:
        copy.wait()


def contract(rows_of, n, copies, held):
    total = None
    for i in range(n):
        copies[i].wait()
        term = nt(rows_of(i), held[i])
        total = term if total is None else total + term
    return total


def pieces(proj, held, done):
    n = held.shape[0]
    copies = [pltpu.make_async_copy(proj.at[:, i * 256 : (i + 1) * 256], held.at[i], done.at[i]) for i in range(n)]
    for copy in copies:
        copy.start()
    return copies


def early_kernel(place, gathered, proj, queries, keys, hidden_ctx, probs, held, done):
    copies = pieces(proj, held, done)
    hidden_ctx[...] = contract(lambda i: gathered[i, 0:MAIN, :], gathered.shape[0], copies, held)
    inv_sqrt = 1.0 / math.sqrt(HEAD_WIDTH)
    kv = pl.multiple_of(place[0] // KEY_VALUE_HEADS * HEAD_WIDTH, HEAD_WIDTH)
    key = keys[:, pl.ds(kv, HEAD_WIDTH)]
    at_key = lax.broadcasted_iota(jnp.int32, (TOKENS, TOKENS), 0)
    at_query = lax.broadcasted_iota(jnp.int32, (TOKENS, TOKENS), 1)
    for h in range(probs.shape[0]):
        scores = nt(key, queries[:, h * 128 : (h + 1) * 128]) * inv_sqrt
        scores = jnp.where(at_key <= at_query, scores, -jnp.inf)
        e = jnp.exp(scores - jnp.max(scores, axis=0, keepdims=True))
        probs[h] = e / jnp.sum(e, axis=0, keepdims=True)


def attention_kernel(place, gathered, rest, proj, queries, keys, values, hidden_ctx, probs, scale, width, sent, shift, held, done, value_held):
    copies = pieces(proj, held, done)
    kv = pl.multiple_of(place[0] // KEY_VALUE_HEADS * HEAD_WIDTH, HEAD_WIDTH)
    fetch = pltpu.make_async_copy(values.at[:, pl.ds(kv, HEAD_WIDTH)], value_held, done.at[held.shape[0]])
    fetch.start()
    row = jnp.zeros((1, 128), F32)
    for i in range(gathered.shape[0]):
        tail = gathered[i, MAIN:ROWS, :].astype(F32)
        row = row + ((tail[0:1, 0:128] + tail[0:1, 128:256]) + tail[1:2, 0:128])
    column = jnp.broadcast_to(row * scale[...] / width[0].astype(F32), (TOKENS, TOKENS)).T
    shift[...] = column
    inv_sqrt = 1.0 / math.sqrt(HEAD_WIDTH)
    key = keys[:, pl.ds(kv, HEAD_WIDTH)]
    stacked = contract(
        lambda i: jnp.concatenate([gathered[i, 0:MAIN, :], rest[i]], axis=0), gathered.shape[0], copies, held
    )
    ctx = stacked[0:TOKENS]
    hidden = jnp.concatenate([hidden_ctx[...], stacked[TOKENS:]], axis=0)
    fetch.wait()
    value = value_held[...]
    n = probs.shape[0]
    key_sum = jnp.zeros((TOKENS, HEAD_WIDTH), F32)
    value_sum = jnp.zeros((TOKENS, HEAD_WIDTH), F32)
    for h in range(n):
        cols = slice(h * 128, (h + 1) * 128)
        grads = (ctx[:, cols] - column * hidden[:, cols]).astype(BF16)
        p = probs[h]
        prob_grads = nt(value, grads)
        delta = jnp.sum(p * prob_grads, axis=0, keepdims=True)
        score_grads = p * (prob_grads - delta) * inv_sqrt
        low = score_grads.astype(BF16)
        sent[:, cols] = nn(score_grads.T.astype(BF16), key).astype(BF16)
        key_sum = key_sum + nn(low, queries[:, cols])
        value_sum = value_sum + nn(p.astype(BF16), grads)
    sent[:, n * 128 : n * 128 + 128] = key_sum.astype(BF16)
    sent[:, n * 128 + 128 : n * 128 + 256] = value_sum.astype(BF16)


def hidden_kernel(full, x, shift, out):
    s = shift[...]
    out[...] = (full[...] - x[...].astype(F32) * jnp.concatenate([s, s], axis=1)).astype(BF16)


def collect_kernel(received, query_out, key_out, value_out):
    n = received.shape[0]
    heads = received.shape[2] - 256
    for i in range(n):
        query_out[:, i * heads : (i + 1) * heads] = received[i, :, 0:heads]
    group = n // KEY_VALUE_HEADS
    for g in range(KEY_VALUE_HEADS):
        for out, at in ((key_out, heads), (value_out, heads + 128)):
            parts = [received[g * group + r, :, at : at + 128].astype(F32) for r in range(group)]
            total = parts[0]
            for part in parts[1:]:
                total = total + part
            out[:, g * 128 : (g + 1) * 128] = total.astype(BF16)


def per_device(
    normed_input,
    norm_gain,
    norm_scale,
    out_grad,
    router_weight,
    routed_experts,
    expert_grad,
    gate_grad,
    out_proj,
    query_states,
    rotated_keys,
    value_tensor,
):
    _, _, _, columns = expert_grad.shape
    n_head = lax.axis_size("head")
    n_experts = router_weight.shape[1]
    place = lax.axis_index("head").reshape(1)
    x, ids = normed_input[0], routed_experts[0].T
    gain = norm_gain.reshape(1, columns)
    width = jnp.full((1,), out_proj.shape[1], jnp.int32)

    local = out_proj.shape[0]
    held_pieces = (pltpu.VMEM((n_head, local, columns), BF16), pltpu.SemaphoreType.DMA((n_head + 1,)))
    packed = pack(expert_grad, gate_grad)
    received = lax.all_to_all(packed, "exp", split_axis=0, concat_axis=0, tiled=True)
    received = received.reshape(n_experts * SLOTS, columns)
    early = call(logits_kernel, shape((ROWS, columns), BF16), x, gain, router_weight, ids)
    early = lax.all_gather(early, "head")
    mix, gate_weights = call(
        weights_kernel, (shape((TOKENS, n_experts * SLOTS), BF16), shape((TOPK, TOKENS))),
        early, ids,
    )
    hidden_ctx, probs = call(
        early_kernel,
        (shape((MAIN, local)), shape((local // HEAD_WIDTH, TOKENS, TOKENS))),
        place, early, out_proj, query_states[0], rotated_keys[0],
        far=(2,), scratch=held_pieces,
    )
    late, rest, full = call(
        rows_kernel,
        (pltpu.HBM((ROWS, columns), BF16), pltpu.HBM((n_head, 2 * LEFT, columns), BF16), pltpu.HBM((TOKENS, columns), F32)),
        received, mix, gate_weights, ids, router_weight, x, gain, norm_scale, out_grad[0],
        far_out=True,
        scratch=(
            pltpu.VMEM((ROWS, columns), BF16), pltpu.VMEM((2 * LEFT, columns), BF16),
            pltpu.VMEM((TOKENS, columns), F32), pltpu.SemaphoreType.DMA((n_head + 3,)),
        ),
    )
    rest = lax.all_to_all(rest, "head", split_axis=0, concat_axis=0, tiled=True)
    late = lax.all_gather(late, "head")
    grads, shift = call(
        attention_kernel,
        (shape((TOKENS, local + 256), BF16), shape((TOKENS, TOKENS))),
        place, late, rest, out_proj, query_states[0], rotated_keys[0], value_tensor[0],
        hidden_ctx, probs, norm_scale, width,
        far=(3, 6), scratch=held_pieces + (pltpu.VMEM((TOKENS, HEAD_WIDTH), BF16),),
    )
    grad_hidden = call(hidden_kernel, shape((TOKENS, columns), BF16), full, x, shift)
    tokens = TOKENS // n_head
    returned = lax.all_to_all(
        grads.reshape(n_head, tokens, local + 256), "head", split_axis=0, concat_axis=0, tiled=True
    )
    query_out, key_out, value_out = call(
        collect_kernel,
        (shape((tokens, n_head * local), BF16), shape((tokens, 512), BF16), shape((tokens, 512), BF16)),
        returned,
    )
    return (grad_hidden[None], query_out[None], key_out[None], value_out[None])


def solution(mesh):
    placed = (
        P("exp", None, "head"),
        P("head"),
        P("exp", None),
        P("exp", None, "head"),
        P("head", None),
        P("exp", None, None),
        P("exp", None, None, "head"),
        P("exp", None, None),
        P("head", None),
        P("exp", None, "head"),
        P("exp", None, None),
        P("exp", None, None),
    )
    return jax.shard_map(
        per_device,
        mesh=mesh,
        in_specs=placed,
        out_specs=(
            P("exp", None, "head"),
            P("exp", "head", None),
            P("exp", "head", None),
            P("exp", "head", None),
        ),
        check_vma=False,
    )
```

```python
import math

import jax
import jax.numpy as jnp
from jax import lax
from jax.experimental import pallas as pl
from jax.experimental.pallas import tpu as pltpu
from jax.sharding import PartitionSpec as P


HEAD_WIDTH = 128
KEY_VALUE_HEADS = 4
TOPK = 8
F32 = jnp.float32
BF16 = jnp.bfloat16
TOKENS = 128
SLOTS = 16
ROWS = 136
TAIL = 136
GRANT = 24 * 2**20


def call(kernel, outs, *args, far=(), far_out=(), scratch=()):
    specs = [
        pl.BlockSpec(
            memory_space=pltpu.SMEM if a.dtype == jnp.int32 and a.size == 1 else pltpu.HBM if i in far else pltpu.VMEM
        )
        for i, a in enumerate(args)
    ]
    args = [pltpu.with_memory_space_constraint(a, pltpu.HBM) if i in far else a for i, a in enumerate(args)]
    one = isinstance(outs, jax.ShapeDtypeStruct)
    vm, hbm = pl.BlockSpec(memory_space=pltpu.VMEM), pl.BlockSpec(memory_space=pltpu.HBM)
    return pl.pallas_call(
        kernel,
        out_shape=outs,
        in_specs=specs,
        out_specs=vm if one else tuple(hbm if i in far_out else vm for i in range(len(outs))),
        scratch_shapes=scratch,
        compiler_params=pltpu.CompilerParams(vmem_limit_bytes=GRANT),
    )(*args)


def shape(s, d=F32):
    return jax.ShapeDtypeStruct(s, d)


def nn(a, b):
    return lax.dot_general(a, b, (((1,), (0,)), ((), ())), preferred_element_type=F32)


def nt(a, b):
    return lax.dot_general(a, b, (((1,), (1,)), ((), ())), preferred_element_type=F32)


def high_low(v):
    high = v.astype(BF16)
    return high, (v - high.astype(F32)).astype(BF16)


def three(v):
    a = v.astype(BF16)
    rest = v - a.astype(F32)
    b = rest.astype(BF16)
    return a, b, (rest - b.astype(F32)).astype(BF16)


def logits_kernel(x, gain, router, ids, sent):
    xv = x[...]
    scaled = xv.astype(F32) * gain[...]
    logits = nn(scaled.astype(BF16), router[...]).T
    experts = lax.broadcasted_iota(jnp.int32, logits.shape, 0)
    rows = []
    for k in range(TOPK):
        rows.append(jnp.sum(jnp.where(ids[k : k + 1, :] == experts, logits, 0.0), axis=0, keepdims=True))
    a, b = high_low(jnp.concatenate(rows, axis=0))
    sent[0:TOKENS, :] = xv
    sent[TOKENS:ROWS, 0:128] = a
    sent[TOKENS:ROWS, 128:256] = b


def picks_kernel(own, total_out):
    total = jnp.zeros((8, 128), F32)
    for i in range(own.shape[0]):
        both = own[i, TOKENS:ROWS, :].astype(F32)
        total = total + (both[:, 0:128] + both[:, 128:256])
    total_out[...] = total


def weights_kernel(own, other, ids, mix, dense, rank):
    total = own[...] + other[...]
    top = jnp.max(total, axis=0, keepdims=True)
    e = jnp.exp(total - top)
    gates = e / jnp.sum(e, axis=0, keepdims=True)
    n = dense.shape[0]
    experts = lax.broadcasted_iota(jnp.int32, (n, TOKENS), 0)
    weight = jnp.zeros((n, TOKENS), F32)
    member = jnp.zeros((n, TOKENS), F32)
    for k in range(TOPK):
        hit = ids[k : k + 1, :] == experts
        weight = jnp.where(hit, gates[k : k + 1, :], weight)
        member = jnp.where(hit, 1.0, member)
    t_from = lax.broadcasted_iota(jnp.int32, (TOKENS, TOKENS), 0)
    t_to = lax.broadcasted_iota(jnp.int32, (TOKENS, TOKENS), 1)
    earlier = jnp.where(t_from < t_to, 1.0, 0.0).astype(BF16)
    before = nn(member.astype(BF16), earlier)
    dense[...] = weight
    rank[...] = before
    step = 8
    for g in range(n // step):
        w3 = weight[g * step : (g + 1) * step, :][:, None, :]
        b3 = before[g * step : (g + 1) * step, :][:, None, :]
        slot = lax.broadcasted_iota(jnp.int32, (step, SLOTS, TOKENS), 1).astype(F32)
        block = jnp.where(jnp.broadcast_to(b3, slot.shape) == slot, jnp.broadcast_to(w3, slot.shape), 0.0)
        block = block.reshape(step * SLOTS, TOKENS).T
        mix[:, g * step * SLOTS : (g + 1) * step * SLOTS] = block.astype(BF16)


def rows_kernel(received, mix, dense, rank, router, x, gain, scale, out_grad, sent_out, full, sent, done):
    n = dense.shape[0]
    rows = received[...]
    both = nn(mix[...], rows)
    e_of = lax.broadcasted_iota(jnp.int32, (n, n * SLOTS), 0)
    j_of = lax.broadcasted_iota(jnp.int32, (n, n * SLOTS), 1)
    pick = jnp.where(j_of == e_of * SLOTS + (SLOTS - 1), 1.0, 0.0).astype(BF16)
    table = nn(pick, received[:, 0:128])
    ranks = rank[...]
    slot_grads = jnp.zeros((n, TOKENS), F32)
    for c in range(SLOTS - 1):
        slot_grads = jnp.where(ranks == float(c), table[:, c : c + 1], slot_grads)
    weight = dense[...]
    mean = jnp.sum(weight * slot_grads, axis=0, keepdims=True)
    diff = (weight * (slot_grads - mean)).T
    d_high, d_low = high_low(diff)
    routed = nt(d_high, router[...]) + nt(d_low, router[...])
    grad = both + routed
    s = jnp.broadcast_to(scale[...], (TOKENS, TOKENS)).T
    moved = out_grad[...].astype(F32) + jnp.concatenate([s, s], axis=1) * (gain[...] * grad)
    full[...] = moved
    sent[0:TOKENS, :] = moved.astype(BF16)
    copies = [
        pltpu.make_async_copy(sent.at[0:TOKENS], sent_out.at[i, 0:TOKENS], done.at[i]) for i in range(sent_out.shape[0])
    ]
    for copy in copies:
        copy.start()
    inner_terms = x[...].astype(F32) * gain[...] * grad
    i_high, i_mid, i_low = three(inner_terms)
    ones = jnp.ones((8, 256), BF16)
    inner = (nt(ones, i_high) + nt(ones, i_mid)) + nt(ones, i_low)
    a, b, c = three(inner)
    row = lax.broadcasted_iota(jnp.int32, (8, 256), 0)
    first = jnp.concatenate([a.astype(F32), b.astype(F32)], axis=1)
    second = jnp.concatenate([c.astype(F32), jnp.zeros((8, 128), F32)], axis=1)
    extra = jnp.where(row == 0, first, jnp.where(row == 1, second, 0.0)).astype(BF16)
    sent[TOKENS:TAIL, :] = extra
    for i in range(sent_out.shape[0]):
        at = pltpu.make_async_copy(sent.at[TOKENS:TAIL], sent_out.at[i, TOKENS:TAIL], done.at[len(copies)])
        at.start()
        copies.append(at)
    for copy in copies:
        copy.wait()


def contract(part, proj, core):
    total = None
    for i in range(part.shape[0]):
        at = pl.multiple_of(i * 512 + core * 256, 256)
        term = nt(part[i, 0:TOKENS, :], proj[:, pl.ds(at, 256)])
        total = term if total is None else total + term
    return total


def half_kernel(place, own, proj, out, held, done):
    bands = 2
    size = held.shape[0] // bands
    copies = [
        pltpu.make_async_copy(proj.at[b * size : (b + 1) * size], held.at[b * size : (b + 1) * size], done.at[b])
        for b in range(bands)
    ]
    for copy in copies:
        copy.start()
    for b in range(bands):
        copies[b].wait()
        out[:, b * size : (b + 1) * size] = contract(own, held.at[b * size : (b + 1) * size], place[0] % 2)


def early_kernel(place, own, other, proj, queries, keys, hidden_ctx, probs):
    core = place[0] % 2
    hidden_ctx[...] = contract(own, proj, core) + contract(other, proj, 1 - core)
    inv_sqrt = 1.0 / math.sqrt(HEAD_WIDTH)
    kv = pl.multiple_of(place[0] // KEY_VALUE_HEADS * HEAD_WIDTH, HEAD_WIDTH)
    key = keys[:, pl.ds(kv, HEAD_WIDTH)]
    at_key = lax.broadcasted_iota(jnp.int32, (TOKENS, TOKENS), 0)
    at_query = lax.broadcasted_iota(jnp.int32, (TOKENS, TOKENS), 1)
    for h in range(probs.shape[1] // TOKENS):
        scores = nt(key, queries[:, h * 128 : (h + 1) * 128]) * inv_sqrt
        scores = jnp.where(at_key <= at_query, scores, -jnp.inf)
        e = jnp.exp(scores - jnp.max(scores, axis=0, keepdims=True))
        probs[:, h * TOKENS : (h + 1) * TOKENS] = e / jnp.sum(e, axis=0, keepdims=True)


def attention_kernel(place, own, other, half, proj, queries, keys, values, hidden_ctx, probs, scale, width, sent, shift):
    core = place[0] % 2
    row = jnp.zeros((1, 128), F32)
    for part in (own, other):
        for i in range(part.shape[0]):
            tail = part[i, TOKENS:TAIL, :].astype(F32)
            row = row + ((tail[0:1, 0:128] + tail[0:1, 128:256]) + tail[1:2, 0:128])
    column = jnp.broadcast_to(row * scale[...] / width[0].astype(F32), (TOKENS, TOKENS)).T
    shift[...] = column
    inv_sqrt = 1.0 / math.sqrt(HEAD_WIDTH)
    kv = pl.multiple_of(place[0] // KEY_VALUE_HEADS * HEAD_WIDTH, HEAD_WIDTH)
    key = keys[:, pl.ds(kv, HEAD_WIDTH)]
    value = values[:, pl.ds(kv, HEAD_WIDTH)]
    ctx = half[...] + contract(other, proj, 1 - core)
    n = hidden_ctx.shape[1] // HEAD_WIDTH
    stack = lambda v: jnp.concatenate([v[:, h * 128 : (h + 1) * 128] for h in range(n)], axis=0)
    wide = jnp.concatenate([column] * n, axis=1)
    grads = stack((ctx - wide * hidden_ctx[...]).astype(BF16))
    p = probs[...]
    prob_grads = nt(value, grads)
    delta = jnp.sum(p * prob_grads, axis=0, keepdims=True)
    score_grads = p * (prob_grads - delta) * inv_sqrt
    query_grads = nn(score_grads.T.astype(BF16), key).astype(BF16)
    for h in range(n):
        sent[:, h * 128 : (h + 1) * 128] = query_grads[h * 128 : (h + 1) * 128]
    sent[:, n * 128 : n * 128 + 128] = nn(score_grads.astype(BF16), stack(queries[...])).astype(BF16)
    sent[:, n * 128 + 128 : n * 128 + 256] = nn(p.astype(BF16), grads).astype(BF16)


def hidden_kernel(full, x, shift, out):
    s = shift[...]
    out[...] = (full[...] - x[...].astype(F32) * jnp.concatenate([s, s], axis=1)).astype(BF16)


def collect_kernel(received, query_out, key_out, value_out):
    n = received.shape[0]
    heads = received.shape[2] - 256
    for i in range(n):
        query_out[:, i * heads : (i + 1) * heads] = received[i, :, 0:heads]
    group = n // KEY_VALUE_HEADS
    for g in range(KEY_VALUE_HEADS):
        for out, at in ((key_out, heads), (value_out, heads + 128)):
            parts = [received[g * group + r, :, at : at + 128].astype(F32) for r in range(group)]
            total = parts[0]
            for part in parts[1:]:
                total = total + part
            out[:, g * 128 : (g + 1) * 128] = total.astype(BF16)


def per_device(
    normed_input,
    norm_gain,
    norm_scale,
    out_grad,
    router_weight,
    routed_experts,
    expert_grad,
    gate_grad,
    out_proj,
    query_states,
    rotated_keys,
    value_tensor,
):
    held, sequences, capacity, columns = expert_grad.shape
    n_head = lax.axis_size("head")
    n_experts = router_weight.shape[1]
    cores = [[2 * i + c for i in range(n_head // 2)] for c in range(2)]
    swap = [(i, i ^ 1) for i in range(n_head)]
    place = lax.axis_index("head").reshape(1)
    x, ids = normed_input[0], routed_experts[0].T
    gain = norm_gain.reshape(1, columns)
    width = jnp.full((1,), out_proj.shape[1], jnp.int32)

    local = out_proj.shape[0]
    gates = jnp.pad(gate_grad.transpose(1, 0, 2)[:, :, None, :], ((0, 0), (0, 0), (0, 0), (0, columns - capacity)))
    packed = jnp.concatenate([expert_grad.transpose(1, 0, 2, 3), gates], axis=2)
    packed = packed.reshape(sequences, held * SLOTS, columns)
    received = lax.all_to_all(packed, "exp", split_axis=0, concat_axis=0, tiled=True)
    received = received.reshape(n_experts * SLOTS, columns)
    early = call(logits_kernel, shape((ROWS, columns), BF16), x, gain, router_weight, ids)
    early_own = lax.all_gather(early, "head", axis_index_groups=cores)
    picks = call(picks_kernel, shape((8, 128)), early_own)
    picks_other = lax.ppermute(picks, "head", swap)
    mix, dense, rank = call(
        weights_kernel,
        (shape((TOKENS, n_experts * SLOTS), BF16), shape((n_experts, TOKENS)), shape((n_experts, TOKENS))),
        picks, picks_other, ids,
    )
    late, full = call(
        rows_kernel,
        (pltpu.HBM((n_head // 2, TAIL, columns), BF16), shape((TOKENS, columns))),
        received, mix, dense, rank, router_weight, x, gain, norm_scale, out_grad[0],
        far_out=(0,), scratch=(pltpu.VMEM((TAIL, columns), BF16), pltpu.SemaphoreType.DMA((n_head,))),
    )
    late_own = lax.all_to_all(late, "head", split_axis=0, concat_axis=0, tiled=True, axis_index_groups=cores)
    early_other = lax.ppermute(early_own, "head", swap)
    hidden_ctx, probs = call(
        early_kernel,
        (shape((TOKENS, local)), shape((TOKENS, local // HEAD_WIDTH * TOKENS))),
        place, early_own, early_other, out_proj, query_states[0], rotated_keys[0],
    )
    late_other = lax.ppermute(late_own, "head", swap)
    half, held = call(
        half_kernel, (shape((TOKENS, local)), shape(out_proj.shape, BF16)), place, late_own, out_proj,
        far=(2,), scratch=(pltpu.SemaphoreType.DMA((2,)),),
    )
    grads, shift = call(
        attention_kernel,
        (shape((TOKENS, local + 256), BF16), shape((TOKENS, TOKENS))),
        place, late_own, late_other, half, held, query_states[0], rotated_keys[0], value_tensor[0],
        hidden_ctx, probs, norm_scale, width,
    )
    grad_hidden = call(hidden_kernel, shape((TOKENS, columns), BF16), full, x, shift)
    tokens = TOKENS // n_head
    returned = lax.all_to_all(
        grads.reshape(n_head, tokens, local + 256), "head", split_axis=0, concat_axis=0, tiled=True
    )
    query_out, key_out, value_out = call(
        collect_kernel,
        (shape((tokens, n_head * local), BF16), shape((tokens, 512), BF16), shape((tokens, 512), BF16)),
        returned,
    )
    return (grad_hidden[None], query_out[None], key_out[None], value_out[None])


def solution(mesh):
    placed = (
        P("exp", None, "head"),
        P("head"),
        P("exp", None),
        P("exp", None, "head"),
        P("head", None),
        P("exp", None, None),
        P("exp", None, None, "head"),
        P("exp", None, None),
        P("head", None),
        P("exp", None, "head"),
        P("exp", None, None),
        P("exp", None, None),
    )
    return jax.shard_map(
        per_device,
        mesh=mesh,
        in_specs=placed,
        out_specs=(
            P("exp", None, "head"),
            P("exp", "head", None),
            P("exp", "head", None),
            P("exp", "head", None),
        ),
        check_vma=False,
    )
```

```python
import math

import jax
import jax.numpy as jnp
from jax import lax
from jax.experimental import pallas as pl
from jax.experimental.pallas import tpu as pltpu
from jax.sharding import PartitionSpec as P


HEAD_WIDTH = 128
KEY_VALUE_HEADS = 4
TOPK = 8
F32 = jnp.float32
BF16 = jnp.bfloat16
TOKENS = 128
SLOTS = 16
MAIN = 112
LEFT = TOKENS - MAIN
ROWS = MAIN + 8
TAIL = 136
GRANT = 24 * 2**20


def call(kernel, outs, *args, far=(), far_out=(), scratch=()):
    specs = [
        pl.BlockSpec(
            memory_space=pltpu.SMEM if a.dtype == jnp.int32 and a.size == 1 else pltpu.HBM if i in far else pltpu.VMEM
        )
        for i, a in enumerate(args)
    ]
    args = [pltpu.with_memory_space_constraint(a, pltpu.HBM) if i in far else a for i, a in enumerate(args)]
    one = isinstance(outs, jax.ShapeDtypeStruct)
    vm, hbm = pl.BlockSpec(memory_space=pltpu.VMEM), pl.BlockSpec(memory_space=pltpu.HBM)
    return pl.pallas_call(
        kernel,
        out_shape=outs,
        in_specs=specs,
        out_specs=vm if one else tuple(hbm if i in far_out else vm for i in range(len(outs))),
        scratch_shapes=scratch,
        compiler_params=pltpu.CompilerParams(vmem_limit_bytes=GRANT),
    )(*args)


def shape(s, d=F32):
    return jax.ShapeDtypeStruct(s, d)


def nn(a, b):
    return lax.dot_general(a, b, (((1,), (0,)), ((), ())), preferred_element_type=F32)


def nt(a, b):
    return lax.dot_general(a, b, (((1,), (1,)), ((), ())), preferred_element_type=F32)


def high_low(v):
    high = v.astype(BF16)
    return high, (v - high.astype(F32)).astype(BF16)


def three(v):
    a = v.astype(BF16)
    rest = v - a.astype(F32)
    b = rest.astype(BF16)
    return a, b, (rest - b.astype(F32)).astype(BF16)


def logits_kernel(x, gain, router, ids, sent):
    xv = x[...]
    scaled = xv.astype(F32) * gain[...]
    logits = nn(scaled.astype(BF16), router[...]).T
    experts = lax.broadcasted_iota(jnp.int32, logits.shape, 0)
    rows = []
    for k in range(TOPK):
        rows.append(jnp.sum(jnp.where(ids[k : k + 1, :] == experts, logits, 0.0), axis=0, keepdims=True))
    a, b = high_low(jnp.concatenate(rows, axis=0))
    sent[0:MAIN, :] = xv[0:MAIN]
    sent[MAIN:ROWS, 0:128] = a
    sent[MAIN:ROWS, 128:256] = b


def spread(gates, ids):
    n = gates.shape[1]
    experts = lax.broadcasted_iota(jnp.int32, (n, TOKENS), 0)
    weight = jnp.zeros((n, TOKENS), F32)
    member = jnp.zeros((n, TOKENS), F32)
    for k in range(TOPK):
        hit = ids[k : k + 1, :] == experts
        weight = jnp.where(hit, gates[k : k + 1, :], weight)
        member = jnp.where(hit, 1.0, member)
    t_from = lax.broadcasted_iota(jnp.int32, (TOKENS, TOKENS), 0)
    t_to = lax.broadcasted_iota(jnp.int32, (TOKENS, TOKENS), 1)
    earlier = jnp.where(t_from < t_to, 1.0, 0.0).astype(BF16)
    return weight, nn(member.astype(BF16), earlier)


def weights_kernel(gathered, ids, mix, gates_out):
    total = jnp.zeros((8, 128), F32)
    for i in range(gathered.shape[0]):
        both = gathered[i, MAIN:ROWS, :].astype(F32)
        total = total + (both[:, 0:128] + both[:, 128:256])
    top = jnp.max(total, axis=0, keepdims=True)
    e = jnp.exp(total - top)
    gates = e / jnp.sum(e, axis=0, keepdims=True)
    gates_out[...] = gates
    weight, before = spread(gates, ids)
    step = 8
    for g in range(weight.shape[0] // step):
        w3 = weight[g * step : (g + 1) * step, :][:, None, :]
        b3 = before[g * step : (g + 1) * step, :][:, None, :]
        slot = lax.broadcasted_iota(jnp.int32, (step, SLOTS, TOKENS), 1).astype(F32)
        block = jnp.where(jnp.broadcast_to(b3, slot.shape) == slot, jnp.broadcast_to(w3, slot.shape), 0.0)
        block = block.reshape(step * SLOTS, TOKENS).T
        mix[:, g * step * SLOTS : (g + 1) * step * SLOTS] = block.astype(BF16)


def rows_kernel(received, mix, gates, ids, router, x, gain, scale, out_grad, sent_out, full_out, sent, full, done):
    weight, ranks = spread(gates[...], ids)
    n = weight.shape[0]
    rows = received[...]
    both = nn(mix[...], rows)
    e_of = lax.broadcasted_iota(jnp.int32, (n, n * SLOTS), 0)
    j_of = lax.broadcasted_iota(jnp.int32, (n, n * SLOTS), 1)
    pick = jnp.where(j_of == e_of * SLOTS + (SLOTS - 1), 1.0, 0.0).astype(BF16)
    table = nn(pick, received[:, 0:128])
    slot_grads = jnp.zeros((n, TOKENS), F32)
    for c in range(SLOTS - 1):
        slot_grads = jnp.where(ranks == float(c), table[:, c : c + 1], slot_grads)
    mean = jnp.sum(weight * slot_grads, axis=0, keepdims=True)
    diff = (weight * (slot_grads - mean)).T
    d_high, d_low = high_low(diff)
    routed = nt(d_high, router[...]) + nt(d_low, router[...])
    grad = both + routed
    s = jnp.broadcast_to(scale[...], (TOKENS, TOKENS)).T
    moved = out_grad[...].astype(F32) + jnp.concatenate([s, s], axis=1) * (gain[...] * grad)
    full[...] = moved
    sent[0:TOKENS, :] = moved.astype(BF16)
    copies = [
        pltpu.make_async_copy(sent.at[0:TOKENS], sent_out.at[i, 0:TOKENS], done.at[i]) for i in range(sent_out.shape[0])
    ]
    copies.append(pltpu.make_async_copy(full, full_out, done.at[len(copies)]))
    for copy in copies:
        copy.start()
    inner_terms = x[...].astype(F32) * gain[...] * grad
    i_high, i_mid, i_low = three(inner_terms)
    ones = jnp.ones((8, 256), BF16)
    inner = (nt(ones, i_high) + nt(ones, i_mid)) + nt(ones, i_low)
    a, b, c = three(inner)
    row = lax.broadcasted_iota(jnp.int32, (8, 256), 0)
    first = jnp.concatenate([a.astype(F32), b.astype(F32)], axis=1)
    second = jnp.concatenate([c.astype(F32), jnp.zeros((8, 128), F32)], axis=1)
    extra = jnp.where(row == 0, first, jnp.where(row == 1, second, 0.0)).astype(BF16)
    sent[TOKENS:TAIL, :] = extra
    for i in range(sent_out.shape[0]):
        at = pltpu.make_async_copy(sent.at[TOKENS:TAIL], sent_out.at[i, TOKENS:TAIL], done.at[len(copies)])
        at.start()
        copies.append(at)
    for copy in copies:
        copy.wait()


def contract(rows_of, blocks, proj):
    total = None
    for i, at in blocks:
        term = nt(rows_of(i), proj[:, pl.ds(at, 256)])
        total = term if total is None else total + term
    return total


def stacked(part, left, proj, core):
    blocks = [(i, pl.multiple_of(i * 512 + core * 256, 256)) for i in range(part.shape[0])]
    return contract(
        lambda i: jnp.concatenate([part[i, 0:TOKENS, :], left[2 * i + core]], axis=0), blocks, proj
    )


def half_kernel(place, own, left, proj, out, held, done):
    bands = done.shape[0]
    size = held.shape[0] // bands
    copies = [
        pltpu.make_async_copy(proj.at[b * size : (b + 1) * size], held.at[b * size : (b + 1) * size], done.at[b])
        for b in range(bands)
    ]
    for copy in copies:
        copy.start()
    for b in range(bands):
        copies[b].wait()
        out[:, b * size : (b + 1) * size] = stacked(own, left, held.at[b * size : (b + 1) * size], place[0] % 2)


def early_kernel(place, gathered, proj, queries, keys, hidden_ctx, probs):
    blocks = [(i, i * 256) for i in range(gathered.shape[0])]
    hidden_ctx[...] = contract(lambda i: gathered[i, 0:MAIN, :], blocks, proj)
    inv_sqrt = 1.0 / math.sqrt(HEAD_WIDTH)
    kv = pl.multiple_of(place[0] // KEY_VALUE_HEADS * HEAD_WIDTH, HEAD_WIDTH)
    key = keys[:, pl.ds(kv, HEAD_WIDTH)]
    at_key = lax.broadcasted_iota(jnp.int32, (TOKENS, TOKENS), 0)
    at_query = lax.broadcasted_iota(jnp.int32, (TOKENS, TOKENS), 1)
    for h in range(probs.shape[1] // TOKENS):
        scores = nt(key, queries[:, h * 128 : (h + 1) * 128]) * inv_sqrt
        scores = jnp.where(at_key <= at_query, scores, -jnp.inf)
        e = jnp.exp(scores - jnp.max(scores, axis=0, keepdims=True))
        probs[:, h * TOKENS : (h + 1) * TOKENS] = e / jnp.sum(e, axis=0, keepdims=True)


def attention_kernel(place, own, other, left, half, proj, queries, keys, values, hidden_ctx, probs, scale, width, sent, shift):
    core = place[0] % 2
    row = jnp.zeros((1, 128), F32)
    for part in (own, other):
        for i in range(part.shape[0]):
            tail = part[i, TOKENS:TAIL, :].astype(F32)
            row = row + ((tail[0:1, 0:128] + tail[0:1, 128:256]) + tail[1:2, 0:128])
    column = jnp.broadcast_to(row * scale[...] / width[0].astype(F32), (TOKENS, TOKENS)).T
    shift[...] = column
    inv_sqrt = 1.0 / math.sqrt(HEAD_WIDTH)
    kv = pl.multiple_of(place[0] // KEY_VALUE_HEADS * HEAD_WIDTH, HEAD_WIDTH)
    key = keys[:, pl.ds(kv, HEAD_WIDTH)]
    value = values[:, pl.ds(kv, HEAD_WIDTH)]
    both = half[...] + stacked(other, left, proj, 1 - core)
    ctx = both[0:TOKENS]
    hidden = jnp.concatenate([hidden_ctx[...], both[TOKENS:]], axis=0)
    n = hidden_ctx.shape[1] // HEAD_WIDTH
    stack = lambda v: jnp.concatenate([v[:, h * 128 : (h + 1) * 128] for h in range(n)], axis=0)
    wide = jnp.concatenate([column] * n, axis=1)
    grads = stack((ctx - wide * hidden).astype(BF16))
    p = probs[...]
    prob_grads = nt(value, grads)
    delta = jnp.sum(p * prob_grads, axis=0, keepdims=True)
    score_grads = p * (prob_grads - delta) * inv_sqrt
    query_grads = nn(score_grads.T.astype(BF16), key).astype(BF16)
    for h in range(n):
        sent[:, h * 128 : (h + 1) * 128] = query_grads[h * 128 : (h + 1) * 128]
    sent[:, n * 128 : n * 128 + 128] = nn(score_grads.astype(BF16), stack(queries[...])).astype(BF16)
    sent[:, n * 128 + 128 : n * 128 + 256] = nn(p.astype(BF16), grads).astype(BF16)


def hidden_kernel(full, x, shift, out):
    s = shift[...]
    out[...] = (full[...] - x[...].astype(F32) * jnp.concatenate([s, s], axis=1)).astype(BF16)


def collect_kernel(received, query_out, key_out, value_out):
    n = received.shape[0]
    heads = received.shape[2] - 256
    for i in range(n):
        query_out[:, i * heads : (i + 1) * heads] = received[i, :, 0:heads]
    group = n // KEY_VALUE_HEADS
    for g in range(KEY_VALUE_HEADS):
        for out, at in ((key_out, heads), (value_out, heads + 128)):
            parts = [received[g * group + r, :, at : at + 128].astype(F32) for r in range(group)]
            total = parts[0]
            for part in parts[1:]:
                total = total + part
            out[:, g * 128 : (g + 1) * 128] = total.astype(BF16)


def per_device(
    normed_input,
    norm_gain,
    norm_scale,
    out_grad,
    router_weight,
    routed_experts,
    expert_grad,
    gate_grad,
    out_proj,
    query_states,
    rotated_keys,
    value_tensor,
):
    held, sequences, capacity, columns = expert_grad.shape
    n_head = lax.axis_size("head")
    n_experts = router_weight.shape[1]
    cores = [[2 * i + c for i in range(n_head // 2)] for c in range(2)]
    swap = [(i, i ^ 1) for i in range(n_head)]
    place = lax.axis_index("head").reshape(1)
    x, ids = normed_input[0], routed_experts[0].T
    gain = norm_gain.reshape(1, columns)
    width = jnp.full((1,), out_proj.shape[1], jnp.int32)

    local = out_proj.shape[0]
    gates = jnp.pad(gate_grad.transpose(1, 0, 2)[:, :, None, :], ((0, 0), (0, 0), (0, 0), (0, columns - capacity)))
    packed = jnp.concatenate([expert_grad.transpose(1, 0, 2, 3), gates], axis=2)
    packed = packed.reshape(sequences, held * SLOTS, columns)
    received = lax.all_to_all(packed, "exp", split_axis=0, concat_axis=0, tiled=True)
    received = received.reshape(n_experts * SLOTS, columns)
    early = call(logits_kernel, shape((ROWS, columns), BF16), x, gain, router_weight, ids)
    early = lax.all_gather(early, "head")
    mix, gate_weights = call(
        weights_kernel, (shape((TOKENS, n_experts * SLOTS), BF16), shape((TOPK, TOKENS))), early, ids,
    )
    hidden_ctx, probs = call(
        early_kernel,
        (shape((MAIN, local)), shape((TOKENS, local // HEAD_WIDTH * TOKENS))),
        place, early, out_proj, query_states[0], rotated_keys[0],
    )
    late, full = call(
        rows_kernel,
        (pltpu.HBM((n_head // 2, TAIL, columns), BF16), pltpu.HBM((TOKENS, columns), F32)),
        received, mix, gate_weights, ids, router_weight, x, gain, norm_scale, out_grad[0],
        far_out=(0, 1),
        scratch=(
            pltpu.VMEM((TAIL, columns), BF16), pltpu.VMEM((TOKENS, columns), F32),
            pltpu.SemaphoreType.DMA((n_head + 1,)),
        ),
    )
    late_own = lax.all_to_all(late, "head", split_axis=0, concat_axis=0, tiled=True, axis_index_groups=cores)
    left = lax.all_gather(x[MAIN:TOKENS], "head")
    late_other = lax.ppermute(late_own, "head", swap)
    half, held = call(
        half_kernel, (shape((TOKENS + LEFT, local)), shape(out_proj.shape, BF16)),
        place, late_own, left, out_proj,
        far=(3,), scratch=(pltpu.SemaphoreType.DMA((4,)),),
    )
    grads, shift = call(
        attention_kernel,
        (shape((TOKENS, local + 256), BF16), shape((TOKENS, TOKENS))),
        place, late_own, late_other, left, half, held, query_states[0], rotated_keys[0], value_tensor[0],
        hidden_ctx, probs, norm_scale, width,
    )
    grad_hidden = call(hidden_kernel, shape((TOKENS, columns), BF16), full, x, shift)
    tokens = TOKENS // n_head
    returned = lax.all_to_all(
        grads.reshape(n_head, tokens, local + 256), "head", split_axis=0, concat_axis=0, tiled=True
    )
    query_out, key_out, value_out = call(
        collect_kernel,
        (shape((tokens, n_head * local), BF16), shape((tokens, 512), BF16), shape((tokens, 512), BF16)),
        returned,
    )
    return (grad_hidden[None], query_out[None], key_out[None], value_out[None])


def solution(mesh):
    placed = (
        P("exp", None, "head"),
        P("head"),
        P("exp", None),
        P("exp", None, "head"),
        P("head", None),
        P("exp", None, None),
        P("exp", None, None, "head"),
        P("exp", None, None),
        P("head", None),
        P("exp", None, "head"),
        P("exp", None, None),
        P("exp", None, None),
    )
    return jax.shard_map(
        per_device,
        mesh=mesh,
        in_specs=placed,
        out_specs=(
            P("exp", None, "head"),
            P("exp", "head", None),
            P("exp", "head", None),
            P("exp", "head", None),
        ),
        check_vma=False,
    )
```

```python
import math

import jax
import jax.numpy as jnp
from jax import lax
from jax.experimental import pallas as pl
from jax.experimental.pallas import tpu as pltpu
from jax.sharding import PartitionSpec as P


HEAD_WIDTH = 128
KEY_VALUE_HEADS = 4
TOPK = 8
F32 = jnp.float32
BF16 = jnp.bfloat16
TOKENS = 128
SLOTS = 16
MAIN = 120
LEFT = TOKENS - MAIN
ROWS = MAIN + TOPK - 1
TAIL = 144
STACK = TOKENS + LEFT
GRANT = 24 * 2**20


def call(kernel, outs, *args, far=(), far_out=(), scratch=()):
    specs = [
        pl.BlockSpec(
            memory_space=pltpu.SMEM if a.dtype == jnp.int32 and a.size == 1 else pltpu.HBM if i in far else pltpu.VMEM
        )
        for i, a in enumerate(args)
    ]
    args = [pltpu.with_memory_space_constraint(a, pltpu.HBM) if i in far else a for i, a in enumerate(args)]
    one = isinstance(outs, jax.ShapeDtypeStruct)
    vm, hbm = pl.BlockSpec(memory_space=pltpu.VMEM), pl.BlockSpec(memory_space=pltpu.HBM)
    return pl.pallas_call(
        kernel,
        out_shape=outs,
        in_specs=specs,
        out_specs=vm if one else tuple(hbm if i in far_out else vm for i in range(len(outs))),
        scratch_shapes=scratch,
        compiler_params=pltpu.CompilerParams(vmem_limit_bytes=GRANT),
    )(*args)


def shape(s, d=F32):
    return jax.ShapeDtypeStruct(s, d)


def nn(a, b):
    return lax.dot_general(a, b, (((1,), (0,)), ((), ())), preferred_element_type=F32)


def nt(a, b):
    return lax.dot_general(a, b, (((1,), (1,)), ((), ())), preferred_element_type=F32)


def high_low(v):
    high = v.astype(BF16)
    return high, (v - high.astype(F32)).astype(BF16)


def three(v):
    a = v.astype(BF16)
    rest = v - a.astype(F32)
    b = rest.astype(BF16)
    return a, b, (rest - b.astype(F32)).astype(BF16)


def logits_kernel(x, gain, router, ids, sent):
    xv = x[...]
    scaled = xv.astype(F32) * gain[...]
    logits = nn(scaled.astype(BF16), router[...]).T
    experts = lax.broadcasted_iota(jnp.int32, logits.shape, 0)
    rows = []
    for k in range(TOPK):
        rows.append(jnp.sum(jnp.where(ids[k : k + 1, :] == experts, logits, 0.0), axis=0, keepdims=True))
    a, b = high_low(jnp.concatenate([row - rows[0] for row in rows[1:]], axis=0))
    sent[0, 0:MAIN, :] = xv[0:MAIN]
    sent[0, MAIN:ROWS, 0:128] = a
    sent[0, MAIN:ROWS, 128:256] = b


def spread(gates, ids):
    n = gates.shape[1]
    experts = lax.broadcasted_iota(jnp.int32, (n, TOKENS), 0)
    weight = jnp.zeros((n, TOKENS), F32)
    member = jnp.zeros((n, TOKENS), F32)
    for k in range(TOPK):
        hit = ids[k : k + 1, :] == experts
        weight = jnp.where(hit, gates[k : k + 1, :], weight)
        member = jnp.where(hit, 1.0, member)
    t_from = lax.broadcasted_iota(jnp.int32, (TOKENS, TOKENS), 0)
    t_to = lax.broadcasted_iota(jnp.int32, (TOKENS, TOKENS), 1)
    earlier = jnp.where(t_from < t_to, 1.0, 0.0).astype(BF16)
    return weight, nn(member.astype(BF16), earlier)


def weights_kernel(gathered, ids, mix, gates_out):
    total = jnp.zeros((TOPK - 1, 128), F32)
    for i in range(gathered.shape[0]):
        both = gathered[i, MAIN:ROWS, :].astype(F32)
        total = total + (both[:, 0:128] + both[:, 128:256])
    total = jnp.concatenate([jnp.zeros((1, 128), F32), total], axis=0)
    top = jnp.max(total, axis=0, keepdims=True)
    e = jnp.exp(total - top)
    gates = e / jnp.sum(e, axis=0, keepdims=True)
    gates_out[...] = gates
    weight, before = spread(gates, ids)
    step = 8
    for g in range(weight.shape[0] // step):
        w3 = weight[g * step : (g + 1) * step, :][:, None, :]
        b3 = before[g * step : (g + 1) * step, :][:, None, :]
        slot = lax.broadcasted_iota(jnp.int32, (step, SLOTS, TOKENS), 1).astype(F32)
        block = jnp.where(jnp.broadcast_to(b3, slot.shape) == slot, jnp.broadcast_to(w3, slot.shape), 0.0)
        block = block.reshape(step * SLOTS, TOKENS).T
        mix[:, g * step * SLOTS : (g + 1) * step * SLOTS] = block.astype(BF16)


def rows_kernel(received, mix, gates, ids, router, x, gain, scale, out_grad, sent_out, full_out, sent, full, done):
    weight, ranks = spread(gates[...], ids)
    n = weight.shape[0]
    rows = received[...]
    both = nn(mix[...], rows)
    e_of = lax.broadcasted_iota(jnp.int32, (n, n * SLOTS), 0)
    j_of = lax.broadcasted_iota(jnp.int32, (n, n * SLOTS), 1)
    pick = jnp.where(j_of == e_of * SLOTS + (SLOTS - 1), 1.0, 0.0).astype(BF16)
    table = nn(pick, received[:, 0:128])
    slot_grads = jnp.zeros((n, TOKENS), F32)
    for c in range(SLOTS - 1):
        slot_grads = jnp.where(ranks == float(c), table[:, c : c + 1], slot_grads)
    mean = jnp.sum(weight * slot_grads, axis=0, keepdims=True)
    diff = (weight * (slot_grads - mean)).T
    d_high, d_low = high_low(diff)
    routed = nt(d_high, router[...]) + nt(d_low, router[...])
    grad = both + routed
    s = jnp.broadcast_to(scale[...], (TOKENS, TOKENS)).T
    moved = out_grad[...].astype(F32) + jnp.concatenate([s, s], axis=1) * (gain[...] * grad)
    full[...] = moved
    sent[0:TOKENS, :] = moved.astype(BF16)
    sent[TOKENS:STACK, :] = x[MAIN:TOKENS, :]
    copies = [
        pltpu.make_async_copy(sent.at[0:STACK], sent_out.at[i, 0:STACK], done.at[i]) for i in range(sent_out.shape[0])
    ]
    copies.append(pltpu.make_async_copy(full, full_out, done.at[len(copies)]))
    for copy in copies:
        copy.start()
    inner_terms = x[...].astype(F32) * gain[...] * grad
    i_high, i_mid, i_low = three(inner_terms)
    ones = jnp.ones((8, 256), BF16)
    inner = (nt(ones, i_high) + nt(ones, i_mid)) + nt(ones, i_low)
    a, b, c = three(inner)
    row = lax.broadcasted_iota(jnp.int32, (8, 256), 0)
    first = jnp.concatenate([a.astype(F32), b.astype(F32)], axis=1)
    second = jnp.concatenate([c.astype(F32), jnp.zeros((8, 128), F32)], axis=1)
    extra = jnp.where(row == 0, first, jnp.where(row == 1, second, 0.0)).astype(BF16)
    sent[STACK:TAIL, :] = extra
    for i in range(sent_out.shape[0]):
        at = pltpu.make_async_copy(sent.at[STACK:TAIL], sent_out.at[i, STACK:TAIL], done.at[len(copies)])
        at.start()
        copies.append(at)
    for copy in copies:
        copy.wait()


def contract(rows_of, blocks, proj):
    total = None
    for i, at in blocks:
        term = nt(rows_of(i), proj[:, pl.ds(at, 256)])
        total = term if total is None else total + term
    return total


def stacked(part, proj, core):
    blocks = [(i, pl.multiple_of(i * 512 + core * 256, 256)) for i in range(part.shape[0])]
    return contract(lambda i: part[i, 0:STACK, :], blocks, proj)


def half_kernel(place, own, proj, out, held, done):
    pieces, bands = done.shape[0], 2
    size, wide = held.shape[0] // pieces, held.shape[0] // bands
    copies = [
        pltpu.make_async_copy(proj.at[b * size : (b + 1) * size], held.at[b * size : (b + 1) * size], done.at[b])
        for b in range(pieces)
    ]
    for copy in copies:
        copy.start()
    for b in range(bands):
        for copy in copies[b * pieces // bands : (b + 1) * pieces // bands]:
            copy.wait()
        out[:, b * wide : (b + 1) * wide] = stacked(own, held.at[b * wide : (b + 1) * wide], place[0] % 2)


def early_kernel(place, gathered, proj, queries, keys, hidden_ctx, probs):
    blocks = [(i, i * 256) for i in range(gathered.shape[0])]
    hidden_ctx[...] = contract(lambda i: gathered[i, 0:MAIN, :], blocks, proj)
    inv_sqrt = 1.0 / math.sqrt(HEAD_WIDTH)
    kv = pl.multiple_of(place[0] // KEY_VALUE_HEADS * HEAD_WIDTH, HEAD_WIDTH)
    key = keys[:, pl.ds(kv, HEAD_WIDTH)]
    at_key = lax.broadcasted_iota(jnp.int32, (TOKENS, TOKENS), 0)
    at_query = lax.broadcasted_iota(jnp.int32, (TOKENS, TOKENS), 1)
    for h in range(probs.shape[1] // TOKENS):
        scores = nt(key, queries[:, h * 128 : (h + 1) * 128]) * inv_sqrt
        scores = jnp.where(at_key <= at_query, scores, -jnp.inf)
        e = jnp.exp(scores - jnp.max(scores, axis=0, keepdims=True))
        probs[:, h * TOKENS : (h + 1) * TOKENS] = e / jnp.sum(e, axis=0, keepdims=True)


def attention_kernel(place, own, other, half, proj, queries, keys, values, hidden_ctx, probs, scale, width, sent, shift):
    core = place[0] % 2
    row = jnp.zeros((1, 128), F32)
    for part in (own, other):
        for i in range(part.shape[0]):
            tail = part[i, STACK:TAIL, :].astype(F32)
            row = row + ((tail[0:1, 0:128] + tail[0:1, 128:256]) + tail[1:2, 0:128])
    column = jnp.broadcast_to(row * scale[...] / width[0].astype(F32), (TOKENS, TOKENS)).T
    shift[...] = column
    inv_sqrt = 1.0 / math.sqrt(HEAD_WIDTH)
    kv = pl.multiple_of(place[0] // KEY_VALUE_HEADS * HEAD_WIDTH, HEAD_WIDTH)
    key = keys[:, pl.ds(kv, HEAD_WIDTH)]
    value = values[:, pl.ds(kv, HEAD_WIDTH)]
    both = half[...] + stacked(other, proj, 1 - core)
    ctx = both[0:TOKENS]
    hidden = jnp.concatenate([hidden_ctx[...], both[TOKENS:]], axis=0)
    n = hidden_ctx.shape[1] // HEAD_WIDTH
    stack = lambda v: jnp.concatenate([v[:, h * 128 : (h + 1) * 128] for h in range(n)], axis=0)
    wide = jnp.concatenate([column] * n, axis=1)
    grads = stack((ctx - wide * hidden).astype(BF16))
    p = probs[...]
    prob_grads = nt(value, grads)
    delta = jnp.sum(p * prob_grads, axis=0, keepdims=True)
    score_grads = p * (prob_grads - delta) * inv_sqrt
    query_grads = nn(score_grads.T.astype(BF16), key).astype(BF16)
    for h in range(n):
        sent[:, h * 128 : (h + 1) * 128] = query_grads[h * 128 : (h + 1) * 128]
    sent[:, n * 128 : n * 128 + 128] = nn(score_grads.astype(BF16), stack(queries[...])).astype(BF16)
    sent[:, n * 128 + 128 : n * 128 + 256] = nn(p.astype(BF16), grads).astype(BF16)


def hidden_kernel(full, x, shift, out):
    s = shift[...]
    out[...] = (full[...] - x[...].astype(F32) * jnp.concatenate([s, s], axis=1)).astype(BF16)


def collect_kernel(received, query_out, key_out, value_out):
    n = received.shape[0]
    heads = received.shape[2] - 256
    for i in range(n):
        query_out[:, i * heads : (i + 1) * heads] = received[i, :, 0:heads]
    group = n // KEY_VALUE_HEADS
    for g in range(KEY_VALUE_HEADS):
        for out, at in ((key_out, heads), (value_out, heads + 128)):
            parts = [received[g * group + r, :, at : at + 128].astype(F32) for r in range(group)]
            total = parts[0]
            for part in parts[1:]:
                total = total + part
            out[:, g * 128 : (g + 1) * 128] = total.astype(BF16)


def per_device(
    normed_input,
    norm_gain,
    norm_scale,
    out_grad,
    router_weight,
    routed_experts,
    expert_grad,
    gate_grad,
    out_proj,
    query_states,
    rotated_keys,
    value_tensor,
):
    held, sequences, capacity, columns = expert_grad.shape
    n_head = lax.axis_size("head")
    n_experts = router_weight.shape[1]
    cores = [[2 * i + c for i in range(n_head // 2)] for c in range(2)]
    swap = [(i, i ^ 1) for i in range(n_head)]
    place = lax.axis_index("head").reshape(1)
    x, ids = normed_input[0], routed_experts[0].T
    gain = norm_gain.reshape(1, columns)
    width = jnp.full((1,), out_proj.shape[1], jnp.int32)

    local = out_proj.shape[0]
    gates = jnp.pad(gate_grad.transpose(1, 0, 2)[:, :, None, :], ((0, 0), (0, 0), (0, 0), (0, columns - capacity)))
    packed = jnp.concatenate([expert_grad.transpose(1, 0, 2, 3), gates], axis=2)
    packed = packed.reshape(sequences, held * SLOTS, columns)
    received = lax.all_to_all(packed, "exp", split_axis=0, concat_axis=0, tiled=True)
    received = received.reshape(n_experts * SLOTS, columns)
    early = call(logits_kernel, shape((1, ROWS, columns), BF16), x, gain, router_weight, ids)
    early = lax.all_gather(early, "head", tiled=True)
    mix, gate_weights = call(
        weights_kernel, (shape((TOKENS, n_experts * SLOTS), BF16), shape((TOPK, TOKENS))), early, ids,
    )
    hidden_ctx, probs = call(
        early_kernel,
        (shape((MAIN, local)), shape((TOKENS, local // HEAD_WIDTH * TOKENS))),
        place, early, out_proj, query_states[0], rotated_keys[0],
    )
    late, full = call(
        rows_kernel,
        (pltpu.HBM((n_head // 2, TAIL, columns), BF16), pltpu.HBM((TOKENS, columns), F32)),
        received, mix, gate_weights, ids, router_weight, x, gain, norm_scale, out_grad[0],
        far_out=(0, 1),
        scratch=(
            pltpu.VMEM((TAIL, columns), BF16), pltpu.VMEM((TOKENS, columns), F32),
            pltpu.SemaphoreType.DMA((n_head + 1,)),
        ),
    )
    late_own = lax.all_to_all(late, "head", split_axis=0, concat_axis=0, tiled=True, axis_index_groups=cores)
    late_other = lax.ppermute(late_own, "head", swap)
    half, held = call(
        half_kernel, (shape((STACK, local)), shape(out_proj.shape, BF16)), place, late_own, out_proj,
        far=(2,), scratch=(pltpu.SemaphoreType.DMA((16,)),),
    )
    grads, shift = call(
        attention_kernel,
        (shape((TOKENS, local + 256), BF16), shape((TOKENS, TOKENS))),
        place, late_own, late_other, half, held, query_states[0], rotated_keys[0], value_tensor[0],
        hidden_ctx, probs, norm_scale, width,
    )
    grad_hidden = call(hidden_kernel, shape((TOKENS, columns), BF16), full, x, shift)
    tokens = TOKENS // n_head
    returned = lax.all_to_all(
        grads.reshape(n_head, tokens, local + 256), "head", split_axis=0, concat_axis=0, tiled=True
    )
    query_out, key_out, value_out = call(
        collect_kernel,
        (shape((tokens, n_head * local), BF16), shape((tokens, 512), BF16), shape((tokens, 512), BF16)),
        returned,
    )
    return (grad_hidden[None], query_out[None], key_out[None], value_out[None])


def solution(mesh):
    placed = (
        P("exp", None, "head"),
        P("head"),
        P("exp", None),
        P("exp", None, "head"),
        P("head", None),
        P("exp", None, None),
        P("exp", None, None, "head"),
        P("exp", None, None),
        P("head", None),
        P("exp", None, "head"),
        P("exp", None, None),
        P("exp", None, None),
    )
    return jax.shard_map(
        per_device,
        mesh=mesh,
        in_specs=placed,
        out_specs=(
            P("exp", None, "head"),
            P("exp", "head", None),
            P("exp", "head", None),
            P("exp", "head", None),
        ),
        check_vma=False,
    )
```

```python
import math

import jax
import jax.numpy as jnp
from jax import lax
from jax.experimental import pallas as pl
from jax.experimental.pallas import tpu as pltpu
from jax.sharding import PartitionSpec as P


HEAD_WIDTH = 128
KEY_VALUE_HEADS = 4
TOPK = 8
F32 = jnp.float32
BF16 = jnp.bfloat16
TOKENS = 128
SLOTS = 16
MAIN = 120
LEFT = TOKENS - MAIN
ROWS = MAIN + TOPK - 1
TAIL = 144
STACK = TOKENS + LEFT
KEPT = 256
GRANT = 24 * 2**20


def call(kernel, outs, *args, far=(), far_out=(), scratch=()):
    specs = [
        pl.BlockSpec(
            memory_space=pltpu.SMEM if a.dtype == jnp.int32 and a.size == 1 else pltpu.HBM if i in far else pltpu.VMEM
        )
        for i, a in enumerate(args)
    ]
    args = [pltpu.with_memory_space_constraint(a, pltpu.HBM) if i in far else a for i, a in enumerate(args)]
    one = isinstance(outs, jax.ShapeDtypeStruct)
    vm, hbm = pl.BlockSpec(memory_space=pltpu.VMEM), pl.BlockSpec(memory_space=pltpu.HBM)
    return pl.pallas_call(
        kernel,
        out_shape=outs,
        in_specs=specs,
        out_specs=vm if one else tuple(hbm if i in far_out else vm for i in range(len(outs))),
        scratch_shapes=scratch,
        compiler_params=pltpu.CompilerParams(vmem_limit_bytes=GRANT),
    )(*args)


def shape(s, d=F32):
    return jax.ShapeDtypeStruct(s, d)


def nn(a, b):
    return lax.dot_general(a, b, (((1,), (0,)), ((), ())), preferred_element_type=F32)


def nt(a, b):
    return lax.dot_general(a, b, (((1,), (1,)), ((), ())), preferred_element_type=F32)


def high_low(v):
    high = v.astype(BF16)
    return high, (v - high.astype(F32)).astype(BF16)


def three(v):
    a = v.astype(BF16)
    rest = v - a.astype(F32)
    b = rest.astype(BF16)
    return a, b, (rest - b.astype(F32)).astype(BF16)


def logits_kernel(x, gain, router, ids, sent):
    xv = x[...]
    scaled = xv.astype(F32) * gain[...]
    logits = nn(scaled.astype(BF16), router[...]).T
    experts = lax.broadcasted_iota(jnp.int32, logits.shape, 0)
    rows = []
    for k in range(TOPK):
        rows.append(jnp.sum(jnp.where(ids[k : k + 1, :] == experts, logits, 0.0), axis=0, keepdims=True))
    a, b = high_low(jnp.concatenate([row - rows[0] for row in rows[1:]], axis=0))
    sent[0, 0:MAIN, :] = xv[0:MAIN]
    sent[0, MAIN:ROWS, 0:128] = a
    sent[0, MAIN:ROWS, 128:256] = b


def spread(gates, ids):
    n = gates.shape[1]
    experts = lax.broadcasted_iota(jnp.int32, (n, TOKENS), 0)
    weight = jnp.zeros((n, TOKENS), F32)
    member = jnp.zeros((n, TOKENS), F32)
    for k in range(TOPK):
        hit = ids[k : k + 1, :] == experts
        weight = jnp.where(hit, gates[k : k + 1, :], weight)
        member = jnp.where(hit, 1.0, member)
    t_from = lax.broadcasted_iota(jnp.int32, (TOKENS, TOKENS), 0)
    t_to = lax.broadcasted_iota(jnp.int32, (TOKENS, TOKENS), 1)
    earlier = jnp.where(t_from < t_to, 1.0, 0.0).astype(BF16)
    return weight, nn(member.astype(BF16), earlier)


def weights_kernel(gathered, ids, mix):
    total = jnp.zeros((TOPK - 1, 128), F32)
    for i in range(gathered.shape[0]):
        both = gathered[i, MAIN:ROWS, :].astype(F32)
        total = total + (both[:, 0:128] + both[:, 128:256])
    total = jnp.concatenate([jnp.zeros((1, 128), F32), total], axis=0)
    top = jnp.max(total, axis=0, keepdims=True)
    e = jnp.exp(total - top)
    gates = e / jnp.sum(e, axis=0, keepdims=True)
    weight, before = spread(gates, ids)
    step = 8
    for g in range(weight.shape[0] // step):
        w3 = weight[g * step : (g + 1) * step, :][:, None, :]
        b3 = before[g * step : (g + 1) * step, :][:, None, :]
        slot = lax.broadcasted_iota(jnp.int32, (step, SLOTS, TOKENS), 1).astype(F32)
        block = jnp.where(jnp.broadcast_to(b3, slot.shape) == slot, jnp.broadcast_to(w3, slot.shape), 0.0)
        block = block.reshape(step * SLOTS, TOKENS).T
        mix[0:TOKENS, g * step * SLOTS : (g + 1) * step * SLOTS] = block.astype(BF16)
    n = weight.shape[0]
    e_of = lax.broadcasted_iota(jnp.int32, (n, n * SLOTS), 0)
    j_of = lax.broadcasted_iota(jnp.int32, (n, n * SLOTS), 1)
    mix[TOKENS : TOKENS + n, 0 : n * SLOTS] = jnp.where(j_of == e_of * SLOTS + (SLOTS - 1), 1.0, 0.0).astype(BF16)
    high, low = high_low(weight)
    at = n * SLOTS
    mix[0:n, at : at + 128] = before.astype(BF16)
    mix[0:n, at + 128 : at + 256] = high
    mix[n : 2 * n, at : at + 128] = low
    mix[n : 2 * n, at + 128 : at + 256] = jnp.zeros_like(low)


def rows_kernel(received, mix, router, x, gain, scale, out_grad, sent_out, full_out, sent, full, done):
    n = mix.shape[0] - TOKENS
    at = n * SLOTS
    product = nn(mix[:, 0:at], received[...])
    both = product[0:TOKENS]
    table = product[TOKENS:, 0:128]
    ranks = mix[0:n, at : at + 128].astype(F32)
    weight = mix[0:n, at + 128 : at + 256].astype(F32) + mix[n : 2 * n, at : at + 128].astype(F32)
    slot_grads = jnp.zeros((n, TOKENS), F32)
    for c in range(SLOTS - 1):
        slot_grads = jnp.where(ranks == float(c), table[:, c : c + 1], slot_grads)
    mean = jnp.sum(weight * slot_grads, axis=0, keepdims=True)
    diff = (weight * (slot_grads - mean)).T
    d_high, d_low = high_low(diff)
    routed = nt(d_high, router[...]) + nt(d_low, router[...])
    grad = both + routed
    s = jnp.broadcast_to(scale[...], (TOKENS, TOKENS)).T
    moved = out_grad[...].astype(F32) + jnp.concatenate([s, s], axis=1) * (gain[...] * grad)
    full[...] = moved
    sent[0:TOKENS, :] = moved.astype(BF16)
    sent[TOKENS:STACK, :] = x[MAIN:TOKENS, :]
    copies = [
        pltpu.make_async_copy(sent.at[0:STACK], sent_out.at[i, 0:STACK], done.at[i]) for i in range(sent_out.shape[0])
    ]
    copies.append(pltpu.make_async_copy(full, full_out, done.at[len(copies)]))
    for copy in copies:
        copy.start()
    inner_terms = x[...].astype(F32) * gain[...] * grad
    i_high, i_mid, i_low = three(inner_terms)
    ones = jnp.ones((8, 256), BF16)
    inner = (nt(ones, i_high) + nt(ones, i_mid)) + nt(ones, i_low)
    a, b, c = three(inner)
    row = lax.broadcasted_iota(jnp.int32, (8, 256), 0)
    first = jnp.concatenate([a.astype(F32), b.astype(F32)], axis=1)
    second = jnp.concatenate([c.astype(F32), jnp.zeros((8, 128), F32)], axis=1)
    extra = jnp.where(row == 0, first, jnp.where(row == 1, second, 0.0)).astype(BF16)
    sent[STACK:TAIL, :] = extra
    for i in range(sent_out.shape[0]):
        at = pltpu.make_async_copy(sent.at[STACK:TAIL], sent_out.at[i, STACK:TAIL], done.at[len(copies)])
        at.start()
        copies.append(at)
    for copy in copies:
        copy.wait()


def contract(rows_of, blocks, proj):
    total = None
    for i, at in blocks:
        term = nt(rows_of(i), proj[:, pl.ds(at, 256)])
        total = term if total is None else total + term
    return total


def stacked(part, proj, core):
    blocks = [(i, pl.multiple_of(i * 512 + core * 256, 256)) for i in range(part.shape[0])]
    return contract(lambda i: part[i, 0:STACK, :], blocks, proj)


def keep_kernel(proj, kept, done):
    copy = pltpu.make_async_copy(proj.at[0:KEPT], kept, done)
    copy.start()
    copy.wait()


def half_kernel(place, own, kept, proj, out, held, done):
    size = held.shape[0] // 2
    copies = [
        pltpu.make_async_copy(
            proj.at[KEPT + b * size : KEPT + (b + 1) * size], held.at[b * size : (b + 1) * size], done.at[b]
        )
        for b in range(2)
    ]
    for copy in copies:
        copy.start()
    core = place[0] % 2
    out[:, 0:KEPT] = stacked(own, kept, core)
    for b in range(2):
        copies[b].wait()
        out[:, KEPT + b * size : KEPT + (b + 1) * size] = stacked(own, held.at[b * size : (b + 1) * size], core)


def early_kernel(place, gathered, proj, queries, keys, hidden_ctx, probs):
    blocks = [(i, i * 256) for i in range(gathered.shape[0])]
    hidden_ctx[...] = contract(lambda i: gathered[i, 0:MAIN, :], blocks, proj)
    inv_sqrt = 1.0 / math.sqrt(HEAD_WIDTH)
    kv = pl.multiple_of(place[0] // KEY_VALUE_HEADS * HEAD_WIDTH, HEAD_WIDTH)
    key = keys[:, pl.ds(kv, HEAD_WIDTH)]
    at_key = lax.broadcasted_iota(jnp.int32, (TOKENS, TOKENS), 0)
    at_query = lax.broadcasted_iota(jnp.int32, (TOKENS, TOKENS), 1)
    for h in range(probs.shape[1] // TOKENS):
        scores = nt(key, queries[:, h * 128 : (h + 1) * 128]) * inv_sqrt
        scores = jnp.where(at_key <= at_query, scores, -jnp.inf)
        e = jnp.exp(scores - jnp.max(scores, axis=0, keepdims=True))
        probs[:, h * TOKENS : (h + 1) * TOKENS] = e / jnp.sum(e, axis=0, keepdims=True)


def attention_kernel(place, own, other, half, kept, held, queries, keys, values, hidden_ctx, probs, scale, width, sent_out, shift_out, sent, shift, done):
    core = place[0] % 2
    row = jnp.zeros((1, 128), F32)
    for part in (own, other):
        for i in range(part.shape[0]):
            tail = part[i, STACK:TAIL, :].astype(F32)
            row = row + ((tail[0:1, 0:128] + tail[0:1, 128:256]) + tail[1:2, 0:128])
    column = jnp.broadcast_to(row * scale[...] / width[0].astype(F32), (TOKENS, TOKENS)).T
    shift[...] = column
    copies = [pltpu.make_async_copy(shift, shift_out, done.at[0])]
    copies[0].start()
    inv_sqrt = 1.0 / math.sqrt(HEAD_WIDTH)
    kv = pl.multiple_of(place[0] // KEY_VALUE_HEADS * HEAD_WIDTH, HEAD_WIDTH)
    key = keys[:, pl.ds(kv, HEAD_WIDTH)]
    value = values[:, pl.ds(kv, HEAD_WIDTH)]
    rest = [stacked(other, part, 1 - core) for part in (kept, held)]
    both = half[...] + jnp.concatenate(rest, axis=1)
    ctx = both[0:TOKENS]
    hidden = jnp.concatenate([hidden_ctx[...], both[TOKENS:]], axis=0)
    n = hidden_ctx.shape[1] // HEAD_WIDTH
    stack = lambda v: jnp.concatenate([v[:, h * 128 : (h + 1) * 128] for h in range(n)], axis=0)
    wide = jnp.concatenate([column] * n, axis=1)
    grads = stack((ctx - wide * hidden).astype(BF16))
    p = probs[...]
    prob_grads = nt(value, grads)
    delta = jnp.sum(p * prob_grads, axis=0, keepdims=True)
    score_grads = p * (prob_grads - delta) * inv_sqrt
    query_grads = nn(score_grads.T.astype(BF16), key).astype(BF16)
    for h in range(n):
        sent[:, h * 128 : (h + 1) * 128] = query_grads[h * 128 : (h + 1) * 128]
    edge = n * 128
    copies.append(pltpu.make_async_copy(sent.at[:, 0:edge], sent_out.at[:, 0:edge], done.at[1]))
    copies[1].start()
    sent[:, edge : edge + 128] = nn(score_grads.astype(BF16), stack(queries[...])).astype(BF16)
    sent[:, edge + 128 : edge + 256] = nn(p.astype(BF16), grads).astype(BF16)
    copies.append(pltpu.make_async_copy(sent.at[:, edge : edge + 256], sent_out.at[:, edge : edge + 256], done.at[2]))
    copies[2].start()
    for copy in copies:
        copy.wait()


def hidden_kernel(full, x, shift, out):
    s = shift[...]
    out[...] = (full[...] - x[...].astype(F32) * jnp.concatenate([s, s], axis=1)).astype(BF16)


def collect_kernel(received, query_out, key_out, value_out):
    n = received.shape[0]
    heads = received.shape[2] - 256
    for i in range(n):
        query_out[:, i * heads : (i + 1) * heads] = received[i, :, 0:heads]
    group = n // KEY_VALUE_HEADS
    for g in range(KEY_VALUE_HEADS):
        for out, at in ((key_out, heads), (value_out, heads + 128)):
            parts = [received[g * group + r, :, at : at + 128].astype(F32) for r in range(group)]
            total = parts[0]
            for part in parts[1:]:
                total = total + part
            out[:, g * 128 : (g + 1) * 128] = total.astype(BF16)


def per_device(
    normed_input,
    norm_gain,
    norm_scale,
    out_grad,
    router_weight,
    routed_experts,
    expert_grad,
    gate_grad,
    out_proj,
    query_states,
    rotated_keys,
    value_tensor,
):
    held, sequences, capacity, columns = expert_grad.shape
    n_head = lax.axis_size("head")
    n_experts = router_weight.shape[1]
    cores = [[2 * i + c for i in range(n_head // 2)] for c in range(2)]
    swap = [(i, i ^ 1) for i in range(n_head)]
    place = lax.axis_index("head").reshape(1)
    x, ids = normed_input[0], routed_experts[0].T
    gain = norm_gain.reshape(1, columns)
    width = jnp.full((1,), out_proj.shape[1], jnp.int32)

    local = out_proj.shape[0]
    gates = jnp.pad(gate_grad.transpose(1, 0, 2)[:, :, None, :], ((0, 0), (0, 0), (0, 0), (0, columns - capacity)))
    packed = jnp.concatenate([expert_grad.transpose(1, 0, 2, 3), gates], axis=2)
    packed = packed.reshape(sequences, held * SLOTS, columns)
    received = lax.all_to_all(packed, "exp", split_axis=0, concat_axis=0, tiled=True)
    received = received.reshape(n_experts * SLOTS, columns)
    early = call(logits_kernel, shape((1, ROWS, columns), BF16), x, gain, router_weight, ids)
    early = lax.all_gather(early, "head", tiled=True)
    mix = call(weights_kernel, shape((TOKENS + n_experts, n_experts * SLOTS + 256), BF16), early, ids)
    hidden_ctx, probs = call(
        early_kernel,
        (shape((MAIN, local)), shape((TOKENS, local // HEAD_WIDTH * TOKENS))),
        place, early, out_proj, query_states[0], rotated_keys[0],
    )
    late, full = call(
        rows_kernel,
        (pltpu.HBM((n_head // 2, TAIL, columns), BF16), pltpu.HBM((TOKENS, columns), F32)),
        received, mix, router_weight, x, gain, norm_scale, out_grad[0],
        far_out=(0, 1),
        scratch=(
            pltpu.VMEM((TAIL, columns), BF16), pltpu.VMEM((TOKENS, columns), F32),
            pltpu.SemaphoreType.DMA((n_head + 1,)),
        ),
    )
    late_own = lax.all_to_all(late, "head", split_axis=0, concat_axis=0, tiled=True, axis_index_groups=cores)
    kept = call(
        keep_kernel, shape((KEPT, out_proj.shape[1]), BF16), out_proj,
        far=(0,), scratch=(pltpu.SemaphoreType.DMA(()),),
    )
    late_other = lax.ppermute(late_own, "head", swap)
    half, held = call(
        half_kernel, (shape((STACK, local)), shape((local - KEPT, out_proj.shape[1]), BF16)),
        place, late_own, kept, out_proj,
        far=(3,), scratch=(pltpu.SemaphoreType.DMA((2,)),),
    )
    grads, shift = call(
        attention_kernel,
        (pltpu.HBM((TOKENS, local + 256), BF16), pltpu.HBM((TOKENS, TOKENS), F32)),
        place, late_own, late_other, half, kept, held, query_states[0], rotated_keys[0], value_tensor[0],
        hidden_ctx, probs, norm_scale, width,
        far_out=(0, 1),
        scratch=(
            pltpu.VMEM((TOKENS, local + 256), BF16), pltpu.VMEM((TOKENS, TOKENS), F32),
            pltpu.SemaphoreType.DMA((3,)),
        ),
    )
    grad_hidden = call(hidden_kernel, shape((TOKENS, columns), BF16), full, x, shift)
    tokens = TOKENS // n_head
    returned = lax.all_to_all(
        grads.reshape(n_head, tokens, local + 256), "head", split_axis=0, concat_axis=0, tiled=True
    )
    query_out, key_out, value_out = call(
        collect_kernel,
        (shape((tokens, n_head * local), BF16), shape((tokens, 512), BF16), shape((tokens, 512), BF16)),
        returned,
    )
    return (grad_hidden[None], query_out[None], key_out[None], value_out[None])


def solution(mesh):
    placed = (
        P("exp", None, "head"),
        P("head"),
        P("exp", None),
        P("exp", None, "head"),
        P("head", None),
        P("exp", None, None),
        P("exp", None, None, "head"),
        P("exp", None, None),
        P("head", None),
        P("exp", None, "head"),
        P("exp", None, None),
        P("exp", None, None),
    )
    return jax.shard_map(
        per_device,
        mesh=mesh,
        in_specs=placed,
        out_specs=(
            P("exp", None, "head"),
            P("exp", "head", None),
            P("exp", "head", None),
            P("exp", "head", None),
        ),
        check_vma=False,
    )
```

```python
import math

import jax
import jax.numpy as jnp
from jax import lax
from jax.experimental import pallas as pl
from jax.experimental.pallas import tpu as pltpu
from jax.sharding import PartitionSpec as P


HEAD_WIDTH = 128
KEY_VALUE_HEADS = 4
TOPK = 8
F32 = jnp.float32
BF16 = jnp.bfloat16
TOKENS = 128
SLOTS = 16
MAIN = 120
LEFT = TOKENS - MAIN
ROWS = MAIN + TOPK - 1
TAIL = 144
STACK = TOKENS + LEFT
KEPT = 256
GRANT = 24 * 2**20


def call(kernel, outs, *args, far=(), far_out=(), scratch=()):
    specs = [
        pl.BlockSpec(
            memory_space=pltpu.SMEM if a.dtype == jnp.int32 and a.size == 1 else pltpu.HBM if i in far else pltpu.VMEM
        )
        for i, a in enumerate(args)
    ]
    args = [pltpu.with_memory_space_constraint(a, pltpu.HBM) if i in far else a for i, a in enumerate(args)]
    one = isinstance(outs, jax.ShapeDtypeStruct)
    vm, hbm = pl.BlockSpec(memory_space=pltpu.VMEM), pl.BlockSpec(memory_space=pltpu.HBM)
    return pl.pallas_call(
        kernel,
        out_shape=outs,
        in_specs=specs,
        out_specs=vm if one else tuple(hbm if i in far_out else vm for i in range(len(outs))),
        scratch_shapes=scratch,
        compiler_params=pltpu.CompilerParams(vmem_limit_bytes=GRANT),
    )(*args)


def shape(s, d=F32):
    return jax.ShapeDtypeStruct(s, d)


def nn(a, b):
    return lax.dot_general(a, b, (((1,), (0,)), ((), ())), preferred_element_type=F32)


def nt(a, b):
    return lax.dot_general(a, b, (((1,), (1,)), ((), ())), preferred_element_type=F32)


def high_low(v):
    high = v.astype(BF16)
    return high, (v - high.astype(F32)).astype(BF16)


def three(v):
    a = v.astype(BF16)
    rest = v - a.astype(F32)
    b = rest.astype(BF16)
    return a, b, (rest - b.astype(F32)).astype(BF16)


def slots_kernel(rows, gates_far, out, gates, done):
    held, slots, n, columns = out.shape
    capacity = slots - 1
    fetch = pltpu.make_async_copy(gates_far, gates, done.at[held])
    fetch.start()
    copies = [pltpu.make_async_copy(rows.at[e], out.at[e, 0:capacity], done.at[e]) for e in range(held)]
    for copy in copies:
        copy.start()
    fetch.wait()
    flat = gates[...].astype(F32)
    for e in range(held):
        wide = jnp.concatenate([flat[:, e, :], jnp.zeros((capacity, 128 - n), F32)], axis=1)
        table = jnp.concatenate([wide, jnp.zeros((128 - capacity, 128), F32)], axis=0).T[0:n]
        out[e, capacity, :, 0:128] = table.astype(BF16)
        out[e, capacity, :, 128:columns] = jnp.zeros((n, columns - 128), BF16)
    for copy in copies:
        copy.wait()


def logits_kernel(x, gain, router, ids, sent):
    xv = x[...]
    scaled = xv.astype(F32) * gain[...]
    logits = nn(scaled.astype(BF16), router[...]).T
    experts = lax.broadcasted_iota(jnp.int32, logits.shape, 0)
    rows = []
    for k in range(TOPK):
        rows.append(jnp.sum(jnp.where(ids[k : k + 1, :] == experts, logits, 0.0), axis=0, keepdims=True))
    a, b = high_low(jnp.concatenate([row - rows[0] for row in rows[1:]], axis=0))
    sent[0, 0:MAIN, :] = xv[0:MAIN]
    sent[0, MAIN:ROWS, 0:128] = a
    sent[0, MAIN:ROWS, 128:256] = b


def spread(gates, ids):
    n = gates.shape[1]
    experts = lax.broadcasted_iota(jnp.int32, (n, TOKENS), 0)
    weight = jnp.zeros((n, TOKENS), F32)
    member = jnp.zeros((n, TOKENS), F32)
    for k in range(TOPK):
        hit = ids[k : k + 1, :] == experts
        weight = jnp.where(hit, gates[k : k + 1, :], weight)
        member = jnp.where(hit, 1.0, member)
    t_from = lax.broadcasted_iota(jnp.int32, (TOKENS, TOKENS), 0)
    t_to = lax.broadcasted_iota(jnp.int32, (TOKENS, TOKENS), 1)
    earlier = jnp.where(t_from < t_to, 1.0, 0.0).astype(BF16)
    return weight, nn(member.astype(BF16), earlier)


def weights_kernel(gathered, ids, mix):
    total = jnp.zeros((TOPK - 1, 128), F32)
    for i in range(gathered.shape[0]):
        both = gathered[i, MAIN:ROWS, :].astype(F32)
        total = total + (both[:, 0:128] + both[:, 128:256])
    total = jnp.concatenate([jnp.zeros((1, 128), F32), total], axis=0)
    top = jnp.max(total, axis=0, keepdims=True)
    e = jnp.exp(total - top)
    gates = e / jnp.sum(e, axis=0, keepdims=True)
    weight, before = spread(gates, ids)
    step = 8
    for g in range(weight.shape[0] // step):
        w3 = weight[g * step : (g + 1) * step, :][:, None, :]
        b3 = before[g * step : (g + 1) * step, :][:, None, :]
        slot = lax.broadcasted_iota(jnp.int32, (step, SLOTS, TOKENS), 1).astype(F32)
        block = jnp.where(jnp.broadcast_to(b3, slot.shape) == slot, jnp.broadcast_to(w3, slot.shape), 0.0)
        block = block.reshape(step * SLOTS, TOKENS).T
        mix[0:TOKENS, g * step * SLOTS : (g + 1) * step * SLOTS] = block.astype(BF16)
    n = weight.shape[0]
    e_of = lax.broadcasted_iota(jnp.int32, (n, n * SLOTS), 0)
    j_of = lax.broadcasted_iota(jnp.int32, (n, n * SLOTS), 1)
    mix[TOKENS : TOKENS + n, 0 : n * SLOTS] = jnp.where(j_of == e_of * SLOTS + (SLOTS - 1), 1.0, 0.0).astype(BF16)
    high, low = high_low(weight)
    at = n * SLOTS
    mix[0:n, at : at + 128] = before.astype(BF16)
    mix[0:n, at + 128 : at + 256] = high
    mix[n : 2 * n, at : at + 128] = low
    mix[n : 2 * n, at + 128 : at + 256] = jnp.zeros_like(low)


def rows_kernel(received, mix, router, x, gain, scale, out_grad, sent_out, full_out, sent, full, done):
    n = mix.shape[0] - TOKENS
    at = n * SLOTS
    product = nn(mix[:, 0:at], received[...])
    both = product[0:TOKENS]
    table = product[TOKENS:, 0:128]
    ranks = mix[0:n, at : at + 128].astype(F32)
    weight = mix[0:n, at + 128 : at + 256].astype(F32) + mix[n : 2 * n, at : at + 128].astype(F32)
    slot_grads = jnp.zeros((n, TOKENS), F32)
    for c in range(SLOTS - 1):
        slot_grads = jnp.where(ranks == float(c), table[:, c : c + 1], slot_grads)
    mean = jnp.sum(weight * slot_grads, axis=0, keepdims=True)
    diff = (weight * (slot_grads - mean)).T
    d_high, d_low = high_low(diff)
    routed = nt(d_high, router[...]) + nt(d_low, router[...])
    grad = both + routed
    s = jnp.broadcast_to(scale[...], (TOKENS, TOKENS)).T
    moved = out_grad[...].astype(F32) + jnp.concatenate([s, s], axis=1) * (gain[...] * grad)
    full[...] = moved
    sent[0:TOKENS, :] = moved.astype(BF16)
    sent[TOKENS:STACK, :] = x[MAIN:TOKENS, :]
    copies = [
        pltpu.make_async_copy(sent.at[0:STACK], sent_out.at[i, 0:STACK], done.at[i]) for i in range(sent_out.shape[0])
    ]
    copies.append(pltpu.make_async_copy(full, full_out, done.at[len(copies)]))
    for copy in copies:
        copy.start()
    inner_terms = x[...].astype(F32) * gain[...] * grad
    i_high, i_mid, i_low = three(inner_terms)
    ones = jnp.ones((8, 256), BF16)
    inner = (nt(ones, i_high) + nt(ones, i_mid)) + nt(ones, i_low)
    a, b, c = three(inner)
    row = lax.broadcasted_iota(jnp.int32, (8, 256), 0)
    first = jnp.concatenate([a.astype(F32), b.astype(F32)], axis=1)
    second = jnp.concatenate([c.astype(F32), jnp.zeros((8, 128), F32)], axis=1)
    extra = jnp.where(row == 0, first, jnp.where(row == 1, second, 0.0)).astype(BF16)
    sent[STACK:TAIL, :] = extra
    for i in range(sent_out.shape[0]):
        at = pltpu.make_async_copy(sent.at[STACK:TAIL], sent_out.at[i, STACK:TAIL], done.at[len(copies)])
        at.start()
        copies.append(at)
    for copy in copies:
        copy.wait()


def contract(rows_of, blocks, proj):
    total = None
    for i, at in blocks:
        term = nt(rows_of(i), proj[:, pl.ds(at, 256)])
        total = term if total is None else total + term
    return total


def stacked(part, proj, core):
    blocks = [(i, pl.multiple_of(i * 512 + core * 256, 256)) for i in range(part.shape[0])]
    return contract(lambda i: part[i, 0:STACK, :], blocks, proj)


def keep_kernel(proj, kept, done):
    copy = pltpu.make_async_copy(proj.at[0:KEPT], kept, done)
    copy.start()
    copy.wait()


def half_kernel(place, own, kept, proj, out, held, done):
    size = held.shape[0] // 2
    copies = [
        pltpu.make_async_copy(
            proj.at[KEPT + b * size : KEPT + (b + 1) * size], held.at[b * size : (b + 1) * size], done.at[b]
        )
        for b in range(2)
    ]
    for copy in copies:
        copy.start()
    core = place[0] % 2
    out[:, 0:KEPT] = stacked(own, kept, core)
    for b in range(2):
        copies[b].wait()
        out[:, KEPT + b * size : KEPT + (b + 1) * size] = stacked(own, held.at[b * size : (b + 1) * size], core)


def early_kernel(place, gathered, proj, queries, keys, hidden_ctx, probs):
    blocks = [(i, i * 256) for i in range(gathered.shape[0])]
    hidden_ctx[...] = contract(lambda i: gathered[i, 0:MAIN, :], blocks, proj)
    inv_sqrt = 1.0 / math.sqrt(HEAD_WIDTH)
    kv = pl.multiple_of(place[0] // KEY_VALUE_HEADS * HEAD_WIDTH, HEAD_WIDTH)
    key = keys[:, pl.ds(kv, HEAD_WIDTH)]
    at_key = lax.broadcasted_iota(jnp.int32, (TOKENS, TOKENS), 0)
    at_query = lax.broadcasted_iota(jnp.int32, (TOKENS, TOKENS), 1)
    for h in range(probs.shape[1] // TOKENS):
        scores = nt(key, queries[:, h * 128 : (h + 1) * 128]) * inv_sqrt
        scores = jnp.where(at_key <= at_query, scores, -jnp.inf)
        e = jnp.exp(scores - jnp.max(scores, axis=0, keepdims=True))
        probs[:, h * TOKENS : (h + 1) * TOKENS] = e / jnp.sum(e, axis=0, keepdims=True)


def attention_kernel(place, own, other, half, kept, held, queries, keys, values, hidden_ctx, probs, scale, width, sent_out, shift_out, sent, shift, done):
    core = place[0] % 2
    row = jnp.zeros((1, 128), F32)
    for part in (own, other):
        for i in range(part.shape[0]):
            tail = part[i, STACK:TAIL, :].astype(F32)
            row = row + ((tail[0:1, 0:128] + tail[0:1, 128:256]) + tail[1:2, 0:128])
    column = jnp.broadcast_to(row * scale[...] / width[0].astype(F32), (TOKENS, TOKENS)).T
    shift[...] = column
    copies = [pltpu.make_async_copy(shift, shift_out, done.at[0])]
    copies[0].start()
    inv_sqrt = 1.0 / math.sqrt(HEAD_WIDTH)
    kv = pl.multiple_of(place[0] // KEY_VALUE_HEADS * HEAD_WIDTH, HEAD_WIDTH)
    key = keys[:, pl.ds(kv, HEAD_WIDTH)]
    value = values[:, pl.ds(kv, HEAD_WIDTH)]
    rest = [stacked(other, part, 1 - core) for part in (kept, held)]
    both = half[...] + jnp.concatenate(rest, axis=1)
    ctx = both[0:TOKENS]
    hidden = jnp.concatenate([hidden_ctx[...], both[TOKENS:]], axis=0)
    n = hidden_ctx.shape[1] // HEAD_WIDTH
    stack = lambda v: jnp.concatenate([v[:, h * 128 : (h + 1) * 128] for h in range(n)], axis=0)
    wide = jnp.concatenate([column] * n, axis=1)
    grads = stack((ctx - wide * hidden).astype(BF16))
    p = probs[...]
    prob_grads = nt(value, grads)
    delta = jnp.sum(p * prob_grads, axis=0, keepdims=True)
    score_grads = p * (prob_grads - delta) * inv_sqrt
    query_grads = nn(score_grads.T.astype(BF16), key).astype(BF16)
    for h in range(n):
        sent[:, h * 128 : (h + 1) * 128] = query_grads[h * 128 : (h + 1) * 128]
    edge = n * 128
    copies.append(pltpu.make_async_copy(sent.at[:, 0:edge], sent_out.at[:, 0:edge], done.at[1]))
    copies[1].start()
    sent[:, edge : edge + 128] = nn(score_grads.astype(BF16), stack(queries[...])).astype(BF16)
    sent[:, edge + 128 : edge + 256] = nn(p.astype(BF16), grads).astype(BF16)
    copies.append(pltpu.make_async_copy(sent.at[:, edge : edge + 256], sent_out.at[:, edge : edge + 256], done.at[2]))
    copies[2].start()
    for copy in copies:
        copy.wait()


def hidden_kernel(full, x, shift, out):
    s = shift[...]
    out[...] = (full[...] - x[...].astype(F32) * jnp.concatenate([s, s], axis=1)).astype(BF16)


def collect_kernel(received, query_out, key_out, value_out):
    n = received.shape[0]
    heads = received.shape[2] - 256
    for i in range(n):
        query_out[:, i * heads : (i + 1) * heads] = received[i, :, 0:heads]
    group = n // KEY_VALUE_HEADS
    for g in range(KEY_VALUE_HEADS):
        for out, at in ((key_out, heads), (value_out, heads + 128)):
            parts = [received[g * group + r, :, at : at + 128].astype(F32) for r in range(group)]
            total = parts[0]
            for part in parts[1:]:
                total = total + part
            out[:, g * 128 : (g + 1) * 128] = total.astype(BF16)


def per_device(
    normed_input,
    norm_gain,
    norm_scale,
    out_grad,
    router_weight,
    routed_experts,
    expert_grad,
    gate_grad,
    out_proj,
    query_states,
    rotated_keys,
    value_tensor,
):
    held, sequences, capacity, columns = expert_grad.shape
    n_head = lax.axis_size("head")
    n_experts = router_weight.shape[1]
    cores = [[2 * i + c for i in range(n_head // 2)] for c in range(2)]
    swap = [(i, i ^ 1) for i in range(n_head)]
    place = lax.axis_index("head").reshape(1)
    x, ids = normed_input[0], routed_experts[0].T
    gain = norm_gain.reshape(1, columns)
    width = jnp.full((1,), out_proj.shape[1], jnp.int32)

    local = out_proj.shape[0]
    packed = call(
        slots_kernel, shape((held, SLOTS, sequences, columns), BF16),
        expert_grad.transpose(0, 2, 1, 3), gate_grad.transpose(2, 0, 1),
        far=(0, 1),
        scratch=(pltpu.VMEM((capacity, held, sequences), BF16), pltpu.SemaphoreType.DMA((held + 1,))),
    )
    packed = packed.transpose(2, 0, 1, 3).reshape(sequences, held * SLOTS, columns)
    received = lax.all_to_all(packed, "exp", split_axis=0, concat_axis=0, tiled=True)
    received = received.reshape(n_experts * SLOTS, columns)
    early = call(logits_kernel, shape((1, ROWS, columns), BF16), x, gain, router_weight, ids)
    early = lax.all_gather(early, "head", tiled=True)
    mix = call(weights_kernel, shape((TOKENS + n_experts, n_experts * SLOTS + 256), BF16), early, ids)
    hidden_ctx, probs = call(
        early_kernel,
        (shape((MAIN, local)), shape((TOKENS, local // HEAD_WIDTH * TOKENS))),
        place, early, out_proj, query_states[0], rotated_keys[0],
    )
    late, full = call(
        rows_kernel,
        (pltpu.HBM((n_head // 2, TAIL, columns), BF16), pltpu.HBM((TOKENS, columns), F32)),
        received, mix, router_weight, x, gain, norm_scale, out_grad[0],
        far_out=(0, 1),
        scratch=(
            pltpu.VMEM((TAIL, columns), BF16), pltpu.VMEM((TOKENS, columns), F32),
            pltpu.SemaphoreType.DMA((n_head + 1,)),
        ),
    )
    late_own = lax.all_to_all(late, "head", split_axis=0, concat_axis=0, tiled=True, axis_index_groups=cores)
    kept = call(
        keep_kernel, shape((KEPT, out_proj.shape[1]), BF16), out_proj,
        far=(0,), scratch=(pltpu.SemaphoreType.DMA(()),),
    )
    late_other = lax.ppermute(late_own, "head", swap)
    half, held = call(
        half_kernel, (shape((STACK, local)), shape((local - KEPT, out_proj.shape[1]), BF16)),
        place, late_own, kept, out_proj,
        far=(3,), scratch=(pltpu.SemaphoreType.DMA((2,)),),
    )
    grads, shift = call(
        attention_kernel,
        (pltpu.HBM((TOKENS, local + 256), BF16), pltpu.HBM((TOKENS, TOKENS), F32)),
        place, late_own, late_other, half, kept, held, query_states[0], rotated_keys[0], value_tensor[0],
        hidden_ctx, probs, norm_scale, width,
        far_out=(0, 1),
        scratch=(
            pltpu.VMEM((TOKENS, local + 256), BF16), pltpu.VMEM((TOKENS, TOKENS), F32),
            pltpu.SemaphoreType.DMA((3,)),
        ),
    )
    grad_hidden = call(hidden_kernel, shape((TOKENS, columns), BF16), full, x, shift)
    tokens = TOKENS // n_head
    returned = lax.all_to_all(
        grads.reshape(n_head, tokens, local + 256), "head", split_axis=0, concat_axis=0, tiled=True
    )
    query_out, key_out, value_out = call(
        collect_kernel,
        (shape((tokens, n_head * local), BF16), shape((tokens, 512), BF16), shape((tokens, 512), BF16)),
        returned,
    )
    return (grad_hidden[None], query_out[None], key_out[None], value_out[None])


def solution(mesh):
    placed = (
        P("exp", None, "head"),
        P("head"),
        P("exp", None),
        P("exp", None, "head"),
        P("head", None),
        P("exp", None, None),
        P("exp", None, None, "head"),
        P("exp", None, None),
        P("head", None),
        P("exp", None, "head"),
        P("exp", None, None),
        P("exp", None, None),
    )
    return jax.shard_map(
        per_device,
        mesh=mesh,
        in_specs=placed,
        out_specs=(
            P("exp", None, "head"),
            P("exp", "head", None),
            P("exp", "head", None),
            P("exp", "head", None),
        ),
        check_vma=False,
    )
```
